256 devices in a mesh: samp: 16 (over z, x_hi), win: 4 (over x_lo, core), snp: 4 (over y).
Axes of the slice: x: 4 (x_hi: 2, x_lo: 2; x = x_hi * 2 + x_lo), y: 4, z: 8, core: 2. Of those that a mesh axis runs over, the one named last changes fastest.
Arguments:
- dosages: bfloat16 [8192, 16384], P('samp', ('win', 'snp')), may hold values from 0 to 2
Outputs:
- r_squared: float32 [4, 4096, 4096], P('win', 'samp', 'snp')
- band_r_squared: float32 [4, 1024, 4096], P('win', 'samp', 'snp')
The draws below stay inside these ranges and needn't reach their ends.
All inputs are finite; a program needn't handle non-finite values.
Results may differ from the reference program's by a relative error of at most 0.0003.
Values may be sent and summed in bfloat16 or wider, within the bound.
A program may use at most 128 MiB of HBM per device.

```python
import jax
import jax.numpy as jnp
from jax import lax

WS = 4096
OV = 1024
WINDOWS = 4
SAMPLES = 8192
SNPS = 16384


def draw_dosages(key, part):
    keys = jax.random.split(key, 5)
    span = min(24, SNPS)
    noise = jax.random.normal(keys[0], (SAMPLES, SNPS), jnp.float32)
    smooth = lax.reduce_window(noise, 0.0, lax.add, (1, span), (1, 1), 'SAME') / span ** 0.5
    own_weight = jax.random.uniform(keys[1], (SNPS,), jnp.float32, 0.3, 1.0)
    mix_weight = jax.random.uniform(keys[2], (SNPS,), jnp.float32, 0.5, 2.5)
    people = jax.random.normal(keys[3], (SAMPLES, 1), jnp.float32)
    loading = jax.random.normal(keys[4], (SNPS,), jnp.float32) * 0.6
    latent = noise * own_weight + smooth * mix_weight
    latent = latent + people * loading
    return (2.0 * jax.nn.sigmoid(latent)).astype(jnp.bfloat16)


def setup_inputs(seed: int = 0) -> dict:
    seeds = jax.random.split(jax.random.key(seed), 2)
    return {
        "dosages": draw_dosages(jax.random.fold_in(seeds[1], 71), 0),
    }


var_floor = 0.05


def squared_corr(gram, col_sum, col_sq, row_sum, row_sq, count):
    col_mean = col_sum / count
    row_mean = row_sum / count
    col_var = jnp.maximum(col_sq / count - col_mean * col_mean, var_floor)
    row_var = jnp.maximum(row_sq / count - row_mean * row_mean, var_floor)
    covar = gram / count - col_mean[:, None] * row_mean[None, :]
    return covar * covar / (col_var[:, None] * row_var[None, :])


def column_stats(block):
    wide = block.astype(jnp.float32)
    return jnp.sum(wide, axis=0), jnp.sum(wide * wide, axis=0)


def reference(dosages):
    count = jnp.float32(dosages.shape[0])
    whole_list = []
    band_list = []
    for window in range(WINDOWS):
        geno = dosages[:, window * WS:(window + 1) * WS]
        following = (window + 1) % WINDOWS
        after = dosages[:, following * WS:following * WS + OV]
        win_sum, win_sq = column_stats(geno)
        next_sum, next_sq = column_stats(after)
        gram = jnp.dot(geno.T, geno, preferred_element_type=jnp.float32)
        next_gram = jnp.dot(after.T, geno, preferred_element_type=jnp.float32)
        whole_list.append(squared_corr(gram, win_sum, win_sq, win_sum, win_sq, count))
        band_list.append(squared_corr(next_gram, next_sum, next_sq, win_sum, win_sq, count))
    return jnp.stack(whole_list), jnp.stack(band_list)
```

```python
import jax
import jax.numpy as jnp
from jax import lax
from jax.experimental import pallas as pl
from jax.experimental.pallas import tpu as pltpu
from jax.sharding import PartitionSpec as P

MESH = pl.DeviceIdType.MESH


Z, Y = 8, 4
SAMPLES = 8192
HERE = 1024
HALF = 512
FLOOR = 0.05
POWER = 15
SCALE = 2.0 ** (126.5 / POWER)
FIRST = (0, 64, 128, 192, 256, 320, 384, 448)
ROWS = 64
PARTS = (
    (0, 64, 0, 256), (0, 64, 256, 256), (64, 32, 0, 512), (96, 32, 0, 512), (128, 32, 0, 512), (160, 32, 0, 512),
    (192, 32, 0, 512), (224, 32, 0, 512), (256, 32, 0, 512), (288, 32, 0, 512), (320, 32, 0, 512),
    (352, 32, 0, 512), (384, 32, 0, 512), (416, 32, 0, 512), (448, 32, 0, 512), (480, 32, 0, 512),
    (576, 32, 0, 512), (608, 32, 0, 512), (512, 32, 0, 512), (544, 32, 0, 512),
)

bf16, f32 = jnp.bfloat16, jnp.float32


def coded(w):
    w2 = w * w
    w3 = w2 * w
    w6 = w3 * w3
    w12 = w6 * w6
    return (w12 * w3).astype(bf16)


def decoded(u):
    u = u.astype(f32)
    size = jnp.exp2(jnp.log2(jnp.abs(u)) * (1.0 / POWER))
    return jnp.where(u < 0, -size, size)


def kernel(
    x_hbm, out_hbm, band_hbm,
    x, xt, cols, own, prev, prods, long_in, long_out, short_in, short_out, done,
    st1, st2, st3, st4, rowv, colv, lanes,
    load_sem, x_send, x_recv, p_send, p_recv,
    s1_send, s1_recv, s2_send, s2_recv, s3_send, s3_recv, s4_send, s4_recv,
    d_send, d_recv, r_send, r_recv, c_send, c_recv,
    l_send, l_recv, t_send, t_recv, o_send, o_recv, b_send, b_recv,
):
    samp, win, y = lax.axis_index("samp"), lax.axis_index("win"), lax.axis_index("snp")
    z, hi = samp // 2, samp % 2
    lo, core = win // 2, win % 2

    def dev(z_, hi_, lo_, core_, y_):
        return (2 * z_ + hi_, 2 * lo_ + core_, y_)

    def remote(src, dst, send, recv, to):
        return pltpu.make_async_remote_copy(
            src_ref=src, dst_ref=dst, send_sem=send, recv_sem=recv, device_id=to, device_id_type=MESH
        )

    def go(copy):
        copy.start()

    def bytes_of(ref, sem):
        pltpu.make_async_copy(ref, ref, sem).wait()

    here = dev(z, hi, lo, core, y)
    partner = dev(z, core, 1 - lo, hi, y)
    sibling = dev(z, hi, lo, 1 - core, y)
    up, down = dev(z, hi, lo, core, (y + 1) % Y), dev(z, hi, lo, core, (y + 3) % Y)
    sign = 1 - 2 * core
    fwd, bwd = dev((z + 8 + sign) % Z, hi, lo, core, y), dev((z + 8 - sign) % Z, hi, lo, core, y)
    mine = pl.ds(pl.multiple_of(HALF * core, HALF), HALF)
    by_hi = pl.ds(pl.multiple_of(HALF * hi, HALF), HALF)

    def turn(a):
        xt[pl.ds(128 * a, 128)] = x[:, pl.ds(128 * a, 128)].T

    load = pltpu.make_async_copy(x_hbm, x, load_sem)
    load.start()
    barrier = pltpu.get_barrier_semaphore()
    met = 0
    for k in range(1, Z):
        pl.semaphore_signal(barrier, 1, device_id=dev((z + k) % Z, hi, lo, core, y), device_id_type=MESH)
        met += 1
    for k in range(1, Y):
        pl.semaphore_signal(barrier, 1, device_id=dev(z, hi, lo, core, (y + k) % Y), device_id_type=MESH)
        met += 1
    for k in range(1, 8):
        pl.semaphore_signal(
            barrier, 1, device_id=dev(z, hi ^ (k // 4), lo ^ (k // 2 % 2), core ^ (k % 2), y), device_id_type=MESH
        )
        met += 1
    load.wait()
    turn(0)
    turn(4)

    pl.semaphore_wait(barrier, met)

    def rows_of(q):
        return pl.ds(FIRST[q], ROWS)

    def x_copy(q, i):
        return remote(
            xt.at[pl.ds(HALF * i + FIRST[q], ROWS)], cols.at[2 * y + i, rows_of(q), by_hi],
            x_send, x_recv.at[q], partner,
        )

    def sx(q):
        if q == 2:
            for a in (1, 5, 2, 6, 3, 7):
                turn(a)
        for i in range(2):
            go(x_copy(q, i))

    next_hi, next_lo = 1 - core, jnp.where(core == 0, 1 - lo, lo)

    def prev_copy(c):
        return remote(
            x.at[:, pl.ds(512 * c, 512)], prev.at[by_hi, :], p_send.at[c], p_recv,
            dev(z, next_hi, next_lo, c, y),
        )

    to_self = jnp.logical_and(hi == 0, core == 1)

    def prev_local():
        return pltpu.make_async_copy(x_hbm.at[:, pl.ds(512, 512)], prev.at[by_hi, :], p_recv)

    def pv():
        go(prev_copy(0))
        pl.when(jnp.logical_not(to_self))(lambda: prev_copy(1).start())
        pl.when(to_self)(lambda: prev_local().start())

    def s1_copy(k):
        return remote(
            st1.at[z], st1.at[z], s1_send, s1_recv, dev((z + k) % Z, hi, lo, core, y)
        )

    def d_copy(q, way, i):
        block = cols.at[2 * y + i, rows_of(q), mine]
        return remote(block, block, d_send, d_recv.at[q, way, i], (up, down)[way])

    def r_copy(q, way):
        block = cols.at[2 * ((y + (3, 1)[way]) % Y) + way, rows_of(q), mine]
        return remote(block, block, r_send, r_recv.at[q], (up, down)[way])

    def pair(q, k):
        return cols.at[pl.ds(2 * ((y + k) % Y), 2), rows_of(q), mine]

    def c_copy(q, k):
        return remote(pair(q, k), pair(q, k), c_send, c_recv.at[q, k], sibling)

    def ax(q):
        bytes_of(pair(q, 0), x_recv.at[q])
        go(c_copy(q, 0))

    def da(q):
        for way in range(2):
            go(d_copy(q, way, way))

    def db(q):
        for way in range(2):
            go(d_copy(q, way, 1 - way))

    def re(q, way):
        d_copy(q, way, way).wait_recv()
        go(r_copy(q, way))

    def ne(q, way):
        d_copy(q, way, 1 - way).wait_recv()
        go(c_copy(q, 3 if way == 0 else 1))

    def fa(q):
        bytes_of(pair(q, 0), r_recv.at[q])
        go(c_copy(q, 2))

    def s2_copy(c):
        return remote(
            lanes, st2.at[hi], s2_send, s2_recv, dev(z, core, 1 - lo, c, y)
        )

    def s3_copy(c):
        return remote(
            lanes, st3.at[hi], s3_send.at[c], s3_recv.at[hi], dev(z, next_hi, next_lo, c, y)
        )

    def s4_copy(k):
        return remote(
            st4.at[y], st4.at[y], s4_send, s4_recv, dev(z, hi, lo, core, (y + k) % Y)
        )

    def st_sums():
        @pl.loop(0, 8)
        def _(a):
            v = x[:, pl.ds(pl.multiple_of(128 * a, 128), 128)].astype(f32)
            st1[z, 0, pl.ds(a, 1), :] = jnp.sum(v, axis=0, keepdims=True)
            st1[z, 1, pl.ds(a, 1), :] = jnp.sum(v * v, axis=0, keepdims=True)

        for k in range(1, Z):
            go(s1_copy(k))

    def st_send():
        bytes_of(st1.at[pl.ds(0, Z - 1)], s1_recv)
        total = st1[0]
        for k in range(1, Z):
            total = total + st1[k]
        lanes[0] = total[0]
        lanes[1] = total[1]
        lanes[2] = st1[z, 0]
        for c in range(2):
            go(s2_copy(c))
        go(s3_copy(0))
        pl.when(jnp.logical_not(to_self))(lambda: s3_copy(1).start())

        @pl.when(to_self)
        def _():
            st3[hi] = lanes[...]

    def st_spread():
        bytes_of(st2, s2_recv)
        st4[y] = st2[0] + st2[1]
        for k in range(1, Y):
            go(s4_copy(k))

    def of_sums(parts):
        total, square, local = (parts[k] for k in range(3))
        mean = total * (1.0 / SAMPLES)
        var = jnp.maximum(square * (1.0 / SAMPLES) - mean * mean, FLOOR)
        return mean, 1.0 / jnp.sqrt(var), local

    def st_finish():
        bytes_of(st4.at[pl.ds(0, Y - 1)], s4_recv)

        @pl.loop(0, Y)
        def _(yy):
            mean, inv, local = of_sums(st4[yy])
            e = inv * (SCALE / SAMPLES)
            rowv[yy, 0] = e.T
            rowv[yy, 1] = (local * e).T
            rowv[yy, 2] = (mean * e).T

        def col_vectors(at, parts):
            mean, inv, local = of_sums(parts)
            lanes_of = (inv, mean * inv, (local - HERE * mean) * inv)
            for n, t in enumerate(lanes_of):
                half = jnp.where(core == 0, t[:4], t[4:])
                for j in range(4):
                    colv[at, n, :, pl.ds(128 * j, 128)] = half[j : j + 1]

        col_vectors(0, st4[y])
        for h in range(2):
            there = pltpu.make_async_copy(st3.at[h], st3.at[h], s3_recv.at[h])
            if h == 0:
                pl.when(jnp.logical_not(to_self))(there.wait)
            else:
                there.wait()
        col_vectors(1, st3[0] + st3[1])

    def st(k):
        (st_sums, st_send, st_spread, st_finish)[k]()

    def ow(m):
        for q in range(len(FIRST)):
            if m == FIRST[q] // 128:
                c_copy(q, 0).wait_recv()
        own[:, pl.ds(128 * m, 128)] = cols[2 * y + core, pl.ds(128 * m, 128)].T

    def products(left, right, size, yy, tiles, roots, at, inside, to, part):
        g = lax.dot_general(
            left.reshape(2 * size, HERE), right[:, part], (((1,), (0,)), ((), ())), preferred_element_type=f32
        )
        for i in range(2):
            e, s, m = (rowv[yy, n, pl.ds(inside, size), tiles[i] : tiles[i] + 1] for n in range(3))
            v = [colv[at, n, :, part] for n in range(3)]
            prods[roots[i], pl.ds(to, size), part] = g[size * i : size * i + size] * (e * v[0]) - s * v[1] - m * v[2]

    def pr(q, k, n=None):
        part = pl.ds(0, 512) if n is None else pl.ds(256 * n, 256)
        if q < len(FIRST):
            if k and not n:
                c_copy(q, k).wait_recv()
            yy = (y + k) % Y
            tile, inside = FIRST[q] // 128, FIRST[q] % 128
            left = cols[pl.ds(2 * yy, 2), rows_of(q)]
            products(left, own, ROWS, yy, (tile, 4 + tile), (2 * yy, 2 * yy + 1), 0, inside, FIRST[q], part)
        else:
            if k == 0:
                bytes_of(prev, p_recv)
            left = cols[0:2, pl.ds(128 * k, 128)]
            products(left, prev, 128, 0, (k, 4 + k), (k, 4 + k), 1, 0, 512, part)

    def spot(u):
        row, tall, col, wide = PARTS[u]
        return pl.ds(row, tall), pl.ds(col, wide)

    def l_copy(t, u):
        r, c = spot(u)
        return remote(long_out.at[t, r, c], long_in.at[t, r, c], l_send, l_recv.at[t, u], fwd)

    def t_copy(t, u):
        r, c = spot(u)
        return remote(short_out.at[t, r, c], short_in.at[t, r, c], t_send, t_recv.at[t, u], bwd)

    def L(t, u):
        r, c = spot(u)
        if t:
            l_copy(t - 1, u).wait_recv()
        w = prods[(z + 8 + sign * (4 - t)) % Z, r, c]
        if t:
            w = w + decoded(long_in[t - 1, r, c])
        long_out[t, r, c] = coded(w)
        go(l_copy(t, u))

    def S(t, u):
        r, c = spot(u)
        if t:
            t_copy(t - 1, u).wait_recv()
        w = prods[(z + 8 - sign * (3 - t)) % Z, r, c]
        if t:
            w = w + decoded(short_in[t - 1, r, c])
        short_out[t, r, c] = coded(w)
        go(t_copy(t, u))

    def place(u):
        row, tall, col, wide = PARTS[u]
        span = 256 if row < 512 else 64
        half = (row % 512) // span
        there = pl.ds(row % 512 % span, tall), pl.ds(pl.multiple_of(HALF * core + col, 128), wide)
        return half, there

    def o_copy(u):
        half, (r, c) = place(u)
        return remote(done.at[spot(u)], out_hbm.at[0, r, c], o_send, o_recv, dev(z, half, 1 - lo, hi, y))

    def b_copy(u):
        half, (r, c) = place(u)
        to = dev(z, half, jnp.where(hi == 1, 1 - lo, lo), 1 - hi, y)
        return remote(done.at[spot(u)], band_hbm.at[0, r, c], b_send.at[half], b_recv, to)

    def b_local(u):
        _, (r, c) = place(u)
        return pltpu.make_async_copy(done.at[spot(u)], band_hbm.at[0, r, c], b_recv)

    def F(u):
        r, c = spot(u)
        l_copy(3, u).wait_recv()
        t_copy(2, u).wait_recv()
        w = prods[z, r, c] + decoded(long_in[3, r, c]) + decoded(short_in[2, r, c])
        done[r, c] = w * w * (1.0 / (SCALE * SCALE))
        if PARTS[u][0] < 512:
            go(o_copy(u))
        elif PARTS[u][0] < 576:
            pl.when(jnp.logical_not(to_self))(lambda: b_copy(u).start())
            pl.when(to_self)(lambda: b_local(u).start())
        else:
            go(b_copy(u))

    plan = [
        (sx, 0), (sx, 1), (sx, 2), (sx, 3), (st, 0), (ax, 0), (da, 0), (db, 0), (st, 1), (sx, 4), (sx, 5), (sx, 6),
        (sx, 7), (ax, 1), (da, 1), (ax, 2), (ow, 0), (ax, 3), (re, 0, 0), (re, 0, 1), (db, 1), (st, 2), (da, 2),
        (ne, 0, 0), (ne, 0, 1), (ow, 1), (ax, 4), (re, 1, 0), (re, 1, 1), (db, 2), (da, 3), (ax, 5), (ax, 6),
        (fa, 0), (ow, 2), (ne, 1, 0), (ne, 1, 1), (ax, 7), (st, 3), (pr, 0, 0, 0), (pr, 0, 1, 0), (pr, 0, 2, 0),
        (re, 2, 0), (re, 2, 1), (db, 3), (da, 4), (pr, 0, 3, 0), (ow, 3), (L, 0, 0), (S, 0, 0), (pr, 0, 0, 1),
        (pr, 0, 1, 1), (pr, 0, 2, 1), (pr, 0, 3, 1), (L, 0, 1), (fa, 1), (S, 0, 1), (pr, 1, 0), (pr, 1, 1),
        (pr, 1, 3), (pr, 2, 0), (ne, 2, 0), (ne, 2, 1), (pr, 3, 0), (pr, 1, 2), (L, 0, 2), (S, 0, 2), (L, 0, 3),
        (S, 0, 3), (pr, 4, 0), (pr, 5, 0), (re, 3, 0), (re, 3, 1), (db, 4), (da, 5), (L, 1, 0), (S, 1, 0),
        (pr, 2, 3), (pr, 2, 1), (L, 1, 1), (S, 1, 1), (pr, 6, 0), (fa, 2), (pr, 7, 0), (pv,), (ne, 3, 0), (ne, 3, 1),
        (pr, 2, 2), (L, 1, 2), (S, 1, 2), (L, 0, 4), (S, 0, 4), (L, 0, 5), (S, 0, 5), (L, 1, 3), (S, 1, 3),
        (re, 4, 0), (re, 4, 1), (db, 5), (da, 6), (L, 2, 0), (S, 2, 0), (pr, 3, 1), (pr, 3, 3), (L, 2, 1), (S, 2, 1),
        (fa, 3), (L, 2, 2), (ne, 4, 0), (ne, 4, 1), (S, 2, 2), (pr, 3, 2), (L, 0, 6), (S, 0, 6), (L, 0, 7),
        (S, 0, 7), (L, 1, 4), (S, 1, 4), (re, 5, 0), (re, 5, 1), (db, 6), (da, 7), (L, 1, 5), (S, 1, 5), (pr, 4, 3),
        (pr, 4, 1), (L, 2, 3), (S, 2, 3), (L, 3, 0), (fa, 4), (L, 3, 1), (ne, 5, 0), (ne, 5, 1), (L, 3, 2),
        (pr, 4, 2), (L, 1, 6), (S, 1, 6), (L, 1, 7), (re, 6, 0), (re, 6, 1), (db, 7), (S, 1, 7), (pr, 5, 3),
        (pr, 5, 1), (L, 2, 4), (S, 2, 4), (fa, 5), (L, 2, 5), (S, 2, 5), (L, 3, 3), (F, 0), (L, 0, 8), (S, 0, 8),
        (ne, 6, 0), (ne, 6, 1), (pr, 5, 2), (F, 1), (S, 2, 6), (L, 0, 9), (S, 0, 9), (F, 2), (S, 2, 7), (L, 0, 10),
        (S, 0, 10), (re, 7, 0), (re, 7, 1), (pr, 6, 3), (L, 2, 6), (pr, 6, 1), (L, 2, 7), (fa, 6), (L, 3, 4),
        (L, 3, 5), (S, 1, 8), (F, 3), (ne, 7, 0), (ne, 7, 1), (L, 0, 11), (S, 0, 11), (pr, 6, 2), (L, 1, 8),
        (S, 1, 9), (L, 1, 9), (fa, 7), (pr, 7, 3), (pr, 7, 1), (L, 1, 10), (S, 1, 10), (L, 3, 6), (pr, 7, 2),
        (L, 3, 7), (S, 2, 8), (pr, 8, 0), (F, 4), (S, 1, 11), (L, 0, 12), (S, 0, 12), (pr, 8, 1), (F, 5), (S, 2, 9),
        (L, 0, 13), (S, 0, 13), (L, 1, 11), (pr, 8, 2), (L, 2, 8), (pr, 8, 3), (L, 2, 9), (S, 2, 10), (L, 2, 10),
        (F, 6), (L, 0, 14), (S, 0, 14), (F, 7), (L, 0, 15), (S, 0, 15), (S, 2, 11), (L, 1, 12), (S, 1, 12),
        (L, 1, 13), (L, 2, 11), (S, 1, 13), (L, 3, 8), (L, 3, 9), (S, 1, 14), (L, 3, 10), (S, 1, 15), (L, 1, 14),
        (L, 1, 15), (S, 2, 12), (L, 2, 12), (S, 2, 13), (L, 2, 13), (L, 3, 11), (S, 2, 14), (F, 8), (S, 2, 15),
        (L, 0, 16), (S, 0, 16), (F, 9), (L, 0, 17), (S, 0, 17), (F, 10), (L, 0, 18), (S, 0, 18), (L, 2, 14),
        (L, 2, 15), (L, 3, 12), (L, 3, 13), (F, 11), (L, 0, 19), (S, 0, 19), (S, 1, 16), (L, 1, 16), (L, 1, 17),
        (S, 1, 17), (S, 1, 18), (L, 1, 18), (L, 3, 14), (L, 3, 15), (F, 12), (F, 13), (S, 1, 19), (L, 1, 19),
        (S, 2, 16), (L, 2, 16), (S, 2, 17), (L, 2, 17), (S, 2, 18), (L, 2, 18), (F, 14), (F, 15), (S, 2, 19),
        (L, 2, 19), (L, 3, 16), (L, 3, 17), (L, 3, 18), (L, 3, 19), (F, 16), (F, 17), (F, 18), (F, 19),
    ]
    for step, *at in plan:
        with jax.named_scope("_".join((step.__name__, *map(str, at)))):
            step(*at)

    def ends():
        bytes_of(xt, x_send)
        bytes_of(cols.at[pl.ds(0, 4), :, mine], d_send)
        bytes_of(cols.at[pl.ds(0, 2), :, mine], r_send)
        bytes_of(cols.at[:, :, mine], c_send)
        bytes_of(st1.at[pl.ds(0, Z - 1)], s1_send)
        bytes_of(st4.at[pl.ds(0, 2)], s2_send)
        bytes_of(st4.at[pl.ds(0, Y - 1)], s4_send)
        bytes_of(long_out, l_send)
        bytes_of(short_out, t_send)
        bytes_of(done.at[pl.ds(0, 512)], o_send)
        bytes_of(done.at[pl.ds(576, 64)], b_send.at[1])
        prev_copy(0).wait_send()
        s3_copy(0).wait_send()

        @pl.when(jnp.logical_not(to_self))
        def _():
            prev_copy(1).wait_send()
            s3_copy(1).wait_send()
            bytes_of(done.at[pl.ds(512, 64)], b_send.at[0])

    def outs():
        bytes_of(out_hbm, o_recv)
        bytes_of(band_hbm, b_recv)

    for step in (ends, outs):
        with jax.named_scope(step.__name__):
            step()


def shards(dosages):
    hbm = pl.BlockSpec(memory_space=pl.ANY)
    dma = pltpu.SemaphoreType.DMA
    n = len(FIRST)
    return pl.pallas_call(
        kernel,
        name="ld",
        out_shape=(
            jax.ShapeDtypeStruct((1, 256, 1024), f32),
            jax.ShapeDtypeStruct((1, 64, 1024), f32),
        ),
        in_specs=[pl.BlockSpec(memory_space=pltpu.HBM)],
        out_specs=(hbm, hbm),
        scratch_shapes=[
            pltpu.VMEM((HALF, 1024), bf16),
            pltpu.VMEM((1024, HALF), bf16),
            pltpu.VMEM((Z, 512, HERE), bf16),
            pltpu.VMEM((HERE, 512), bf16),
            pltpu.VMEM((HERE, 512), bf16),
            pltpu.VMEM((Z, 640, 512), f32),
            pltpu.VMEM((4, 640, 512), bf16),
            pltpu.VMEM((4, 640, 512), bf16),
            pltpu.VMEM((3, 640, 512), bf16),
            pltpu.VMEM((3, 640, 512), bf16),
            pltpu.VMEM((640, 512), f32),
            pltpu.VMEM((Z, 2, 8, 128), f32),
            pltpu.VMEM((2, 3, 8, 128), f32),
            pltpu.VMEM((2, 3, 8, 128), f32),
            pltpu.VMEM((Y, 3, 8, 128), f32),
            pltpu.VMEM((Y, 3, 128, 8), f32),
            pltpu.VMEM((2, 3, 1, 512), f32),
            pltpu.VMEM((3, 8, 128), f32),
            dma,
            dma, dma((n,)), dma((2,)), dma,
            dma, dma, dma, dma, dma((2,)), dma((2,)), dma, dma,
            dma, dma((n, 2, 2)), dma, dma((n,)), dma, dma((n, 4)),
            dma, dma((4, len(PARTS))), dma, dma((3, len(PARTS))),
            dma, dma, dma((2,)), dma,
        ],
        compiler_params=pltpu.CompilerParams(has_side_effects=True, collective_id=0, vmem_limit_bytes=44 * 2**20),
    )(pltpu.with_memory_space_constraint(dosages, pltpu.HBM))


def solution(mesh):
    return jax.shard_map(
        shards,
        mesh=mesh,
        in_specs=(P("samp", ("win", "snp")),),
        out_specs=(P("win", "samp", "snp"), P("win", "samp", "snp")),
        check_vma=False,
    )
```

```python
import jax
import jax.numpy as jnp
from jax import lax
from jax.experimental import pallas as pl
from jax.experimental.pallas import tpu as pltpu
from jax.sharding import PartitionSpec as P

MESH = pl.DeviceIdType.MESH


Z, Y = 8, 4
SAMPLES = 8192
HERE = 1024
HALF = 512
FLOOR = 0.05
POWER = 15
SCALE = 2.0 ** (126.5 / POWER)
FIRST = (0, 32, 64, 128, 192, 256, 320, 384, 448)
ROWS = (32, 32, 64, 64, 64, 64, 64, 64, 64)
PARTS = (
    (0, 32, 0, 256), (0, 32, 256, 256), (32, 32, 0, 256), (32, 32, 256, 256), (64, 32, 0, 512), (96, 32, 0, 512),
    (128, 32, 0, 512), (160, 32, 0, 512), (192, 32, 0, 512), (224, 32, 0, 512), (256, 32, 0, 512),
    (288, 32, 0, 512), (320, 32, 0, 512), (352, 32, 0, 512), (384, 32, 0, 512), (416, 32, 0, 512),
    (448, 32, 0, 512), (480, 32, 0, 512), (576, 32, 0, 512), (608, 32, 0, 512), (512, 32, 0, 512),
    (544, 32, 0, 512),
)
TURN = sum(row < 128 for row in FIRST)
LONG_AT = (
    (0, 2, 3, 4, 5, 6, 11, 12, 2, 15, 0, 7, 3, 4, 15, 14, 17, 11, 0, 7, 8, 12),
    (1, 0, 8, 9, 10, 13, 5, 16, 8, 9, 5, 1, 6, 16, 9, 3, 1, 13, 2, 15, 6, 16),
    (7, 14, 1, 3, 4, 17, 6, 12, 13, 2, 10, 18, 4, 19, 14, 5, 10, 0, 18, 11, 17, 20),
)
SHORT_AT = (
    (0, 2, 3, 4, 5, 6, 10, 12, 5, 3, 8, 7, 12, 10, 3, 4, 8, 7, 6, 13, 14, 15),
    (1, 0, 7, 8, 9, 11, 4, 0, 9, 6, 11, 2, 5, 0, 9, 1, 2, 11, 10, 12, 16, 3),
)

bf16, f32 = jnp.bfloat16, jnp.float32


def coded(w):
    w2 = w * w
    w3 = w2 * w
    w6 = w3 * w3
    w12 = w6 * w6
    return (w12 * w3).astype(bf16)


def decoded(u):
    u = u.astype(f32)
    size = jnp.exp2(jnp.log2(jnp.abs(u)) * (1.0 / POWER))
    return jnp.where(u < 0, -size, size)


def kernel(
    x_hbm, out_ref, band_ref,
    x, xt, cols, own, prev, prods, long_in, long_out, short_in, short_out, own_out, ends,
    st1, st2, st3, rowv, colv, lanes,
    load_sem, x_send, x_recv, p_send, p_recv,
    s1_send, s1_recv, s2_send, s2_recv, s3_send, s3_recv,
    d_send, d_recv, r_send, r_recv, c_send, c_recv,
    l_send, l_recv, t_send, t_recv, o_send, b_send, e_recv,
):
    samp, win, y = lax.axis_index("samp"), lax.axis_index("win"), lax.axis_index("snp")
    z, hi = samp // 2, samp % 2
    lo, core = win // 2, win % 2

    def dev(z_, hi_, lo_, core_, y_):
        return (2 * z_ + hi_, 2 * lo_ + core_, y_)

    def remote(src, dst, send, recv, to):
        return pltpu.make_async_remote_copy(
            src_ref=src, dst_ref=dst, send_sem=send, recv_sem=recv, device_id=to, device_id_type=MESH
        )

    def go(copy):
        copy.start()

    def bytes_of(ref, sem):
        pltpu.make_async_copy(ref, ref, sem).wait()

    here = dev(z, hi, lo, core, y)
    partner = dev(z, core, 1 - lo, hi, y)
    sibling = dev(z, hi, lo, 1 - core, y)
    up, down = dev(z, hi, lo, core, (y + 1) % Y), dev(z, hi, lo, core, (y + 3) % Y)
    sign = 1 - 2 * core
    fwd, bwd = dev((z + 8 + sign) % Z, hi, lo, core, y), dev((z + 8 - sign) % Z, hi, lo, core, y)
    mine = pl.ds(pl.multiple_of(HALF * core, HALF), HALF)
    by_hi = pl.ds(pl.multiple_of(HALF * hi, HALF), HALF)

    def turn(a):
        xt[pl.ds(128 * a, 128)] = x[:, pl.ds(128 * a, 128)].T

    def load(first, count, k):
        part = pl.ds(128 * first, 128 * count)
        return pltpu.make_async_copy(x_hbm.at[:, part], x.at[:, part], load_sem.at[k])

    loads = [load(0, 1, 0), load(4, 1, 1), load(1, 3, 2), load(5, 3, 3)]
    for copy in loads:
        copy.start()
    barrier = pltpu.get_barrier_semaphore()
    met = 0
    for k in range(1, Z):
        pl.semaphore_signal(barrier, 1, device_id=dev((z + k) % Z, hi, lo, core, y), device_id_type=MESH)
        met += 1
    for k in range(1, Y):
        pl.semaphore_signal(barrier, 1, device_id=dev(z, hi, lo, core, (y + k) % Y), device_id_type=MESH)
        met += 1
    for k in range(1, 8):
        pl.semaphore_signal(
            barrier, 1, device_id=dev(z, hi ^ (k // 4), lo ^ (k // 2 % 2), core ^ (k % 2), y), device_id_type=MESH
        )
        met += 1
    for k in range(1, Y):
        for other in ((core, 0), (core, 1), (1 - core, None)):
            near = dev(z, other[0], 1 - lo, hi if other[1] is None else other[1], (y + k) % Y)
            pl.semaphore_signal(barrier, 1, device_id=near, device_id_type=MESH)
            met += 1
    for dz in (1, Z - 1):
        for k in range(1, 8):
            near = dev((z + dz) % Z, hi ^ (k // 4), lo ^ (k // 2 % 2), core ^ (k % 2), y)
            pl.semaphore_signal(barrier, 1, device_id=near, device_id_type=MESH)
            met += 1
    for n in range(2):
        loads[n].wait()
        turn(4 * n)

    pl.semaphore_wait(barrier, met)

    def rows_of(q):
        return pl.ds(FIRST[q], ROWS[q])

    def x_copy(q, i):
        return remote(
            xt.at[pl.ds(HALF * i + FIRST[q], ROWS[q])], cols.at[2 * y + i, rows_of(q), by_hi],
            x_send, x_recv.at[q], partner,
        )

    def sx(q):
        if q == TURN:
            for a in (1, 5, 2, 6, 3, 7):
                turn(a)
        for i in range(2):
            go(x_copy(q, i))

    next_hi, next_lo = 1 - core, jnp.where(core == 0, 1 - lo, lo)

    def prev_copy(c):
        return remote(
            x.at[:, pl.ds(512 * c, 512)], prev.at[by_hi, :], p_send.at[c], p_recv,
            dev(z, next_hi, next_lo, c, y),
        )

    to_self = jnp.logical_and(hi == 0, core == 1)

    def prev_local():
        return pltpu.make_async_copy(x_hbm.at[:, pl.ds(512, 512)], prev.at[by_hi, :], p_recv)

    def pv():
        go(prev_copy(0))
        pl.when(jnp.logical_not(to_self))(lambda: prev_copy(1).start())
        pl.when(to_self)(lambda: prev_local().start())

    def s1_copy(k):
        return remote(
            st1.at[z], st1.at[z], s1_send, s1_recv, dev((z + k) % Z, hi, lo, core, y)
        )

    def d_copy(q, way, i):
        block = cols.at[2 * y + i, rows_of(q), mine]
        return remote(block, block, d_send, d_recv.at[q, way ^ i], (up, down)[way])

    def r_copy(q, way):
        block = cols.at[2 * ((y + (3, 1)[way]) % Y) + way, rows_of(q), mine]
        return remote(block, block, r_send, r_recv.at[q], (up, down)[way])

    def pair(q, k):
        return cols.at[pl.ds(2 * ((y + k) % Y), 2), rows_of(q), mine]

    def c_copy(q, k):
        return remote(pair(q, k), pair(q, k), c_send, c_recv.at[q, (0, 1, 2, 1)[k]], sibling)

    def ax(q):
        bytes_of(pair(q, 0), x_recv.at[q])
        go(c_copy(q, 0))

    def da(q):
        for way in range(2):
            go(d_copy(q, way, way))

    def db(q):
        for way in range(2):
            go(d_copy(q, way, 1 - way))

    def re(q):
        bytes_of(pair(q, 0), d_recv.at[q, 0])
        for way in range(2):
            go(r_copy(q, way))

    def ne(q):
        bytes_of(pair(q, 0), d_recv.at[q, 1])
        for k in (1, 3):
            go(c_copy(q, k))

    def fa(q):
        bytes_of(pair(q, 0), r_recv.at[q])
        go(c_copy(q, 2))

    def s2_copy(yy, c):
        return remote(lanes, st2.at[y, hi], s2_send, s2_recv, dev(z, core, 1 - lo, c, yy))

    def s3_copy(c):
        return remote(
            lanes, st3.at[hi], s3_send.at[c], s3_recv.at[hi], dev(z, next_hi, next_lo, c, y)
        )

    def st_sums():
        for n in (2, 3):
            loads[n].wait()

        @pl.loop(0, 8)
        def _(a):
            v = x[:, pl.ds(pl.multiple_of(128 * a, 128), 128)].astype(f32)
            st1[z, 0, pl.ds(a, 1), :] = jnp.sum(v, axis=0, keepdims=True)
            st1[z, 1, pl.ds(a, 1), :] = jnp.sum(v * v, axis=0, keepdims=True)

        for k in range(1, Z):
            go(s1_copy(k))

    def st_send():
        bytes_of(st1.at[pl.ds(0, Z - 1)], s1_recv)
        total = st1[0]
        for k in range(1, Z):
            total = total + st1[k]
        lanes[0] = total[0]
        lanes[1] = total[1]
        lanes[2] = st1[z, 0]
        for c in range(2):
            for k in range(Y):
                go(s2_copy((y + k) % Y, c))
        go(s3_copy(0))
        pl.when(jnp.logical_not(to_self))(lambda: s3_copy(1).start())

        @pl.when(to_self)
        def _():
            st3[hi] = lanes[...]

    def of_sums(parts):
        total, square, local = (parts[k] for k in range(3))
        mean = total * (1.0 / SAMPLES)
        var = jnp.maximum(square * (1.0 / SAMPLES) - mean * mean, FLOOR)
        return mean, 1.0 / jnp.sqrt(var), local

    def st_finish():
        bytes_of(st2, s2_recv)

        @pl.loop(0, Y)
        def _(yy):
            mean, inv, local = of_sums(st2[yy, 0] + st2[yy, 1])
            e = inv * (SCALE / SAMPLES)
            rowv[yy, 0] = e.T
            rowv[yy, 1] = (local * e).T
            rowv[yy, 2] = (mean * e).T

        def col_vectors(at, parts):
            mean, inv, local = of_sums(parts)
            lanes_of = (inv, mean * inv, (local - HERE * mean) * inv)
            for n, t in enumerate(lanes_of):
                half = jnp.where(core == 0, t[:4], t[4:])
                for j in range(4):
                    colv[at, n, :, pl.ds(128 * j, 128)] = half[j : j + 1]

        col_vectors(0, st2[y, 0] + st2[y, 1])
        for h in range(2):
            there = pltpu.make_async_copy(st3.at[h], st3.at[h], s3_recv.at[h])
            if h == 0:
                pl.when(jnp.logical_not(to_self))(there.wait)
            else:
                there.wait()
        col_vectors(1, st3[0] + st3[1])

    def st(k):
        (st_sums, st_send, st_finish)[k]()

    def ow(m):
        for q in range(len(FIRST)):
            if m == (FIRST[q] + ROWS[q] - 1) // 128:
                c_copy(q, 0).wait_recv()
        own[:, pl.ds(128 * m, 128)] = cols[2 * y + core, pl.ds(128 * m, 128)].T

    def products(left, right, size, yy, tiles, roots, at, inside, to, part):
        g = lax.dot_general(
            left.reshape(2 * size, HERE), right[:, part], (((1,), (0,)), ((), ())), preferred_element_type=f32
        )
        for i in range(2):
            e, s, m = (rowv[yy, n, pl.ds(inside, size), tiles[i] : tiles[i] + 1] for n in range(3))
            v = [colv[at, n, :, part] for n in range(3)]
            prods[roots[i], pl.ds(to, size), part] = g[size * i : size * i + size] * (e * v[0]) - s * v[1] - m * v[2]

    def main(q, ks, n):
        part = pl.ds(0, 512) if n is None else pl.ds(256 * n, 256)
        tile, inside = FIRST[q] // 128, FIRST[q] % 128
        for k in ks:
            yy = (y + k) % Y
            left = cols[pl.ds(2 * yy, 2), rows_of(q)]
            products(left, own, ROWS[q], yy, (tile, 4 + tile), (2 * yy, 2 * yy + 1), 0, inside, FIRST[q], part)

    def pn(q, n=None):
        if not n:
            bytes_of(cols.at[pl.ds(0, 4), rows_of(q), mine], c_recv.at[q, 1])
        main(q, (0, 1, 3), n)

    def pa(q, n=None):
        main(q, (0, 1, 2, 3), n)

    def pf(q, n=None):
        if not n:
            c_copy(q, 2).wait_recv()
        main(q, (2,), n)

    def pb():
        bytes_of(prev, p_recv)
        for k in range(4):
            left = cols[0:2, pl.ds(128 * k, 128)]
            products(left, prev, 128, 0, (k, 4 + k), (k, 4 + k), 1, 0, 512, pl.ds(0, 512))

    def spot(u):
        row, tall, col, wide = PARTS[u]
        return pl.ds(row, tall), pl.ds(col, wide)

    def half_of(u):
        row = PARTS[u][0]
        return row // 256 if row < 512 else (row - 512) // 64

    def slot(u):
        return sum(half_of(n) == half_of(u) for n in range(u))

    def home(u, z_):
        if PARTS[u][0] < 512:
            return dev(z_, half_of(u), 1 - lo, hi, y)
        return dev(z_, half_of(u), jnp.where(hi == 1, 1 - lo, lo), 1 - hi, y)

    def at_home(u):
        row, tall, col, wide = PARTS[u]
        return pl.ds(row % 256 if row < 512 else 256 + (row - 512) % 64, tall), pl.ds(col, wide)

    def l_copy(t, u):
        r, c = spot(u)
        if t < 3:
            return remote(long_out.at[t, r, c], long_in.at[t, r, c], l_send, l_recv.at[LONG_AT[t][u]], fwd)
        hr, hc = at_home(u)
        return remote(
            long_out.at[t, r, c], ends.at[0, core, hr, hc], l_send, e_recv.at[slot(u), core],
            home(u, (z + 8 + sign) % Z),
        )

    def t_copy(t, u):
        r, c = spot(u)
        if t < 2:
            return remote(short_out.at[t, r, c], short_in.at[t, r, c], t_send, t_recv.at[SHORT_AT[t][u]], bwd)
        hr, hc = at_home(u)
        return remote(
            short_out.at[t, r, c], ends.at[1, core, hr, hc], t_send, e_recv.at[slot(u), core],
            home(u, (z + 8 - sign) % Z),
        )

    def L(t, u):
        r, c = spot(u)
        if t:
            l_copy(t - 1, u).wait_recv()
        w = prods[(z + 8 + sign * (4 - t)) % Z, r, c]
        if t:
            w = w + decoded(long_in[t - 1, r, c])
        long_out[t, r, c] = coded(w)
        go(l_copy(t, u))

    def S(t, u):
        r, c = spot(u)
        if t:
            t_copy(t - 1, u).wait_recv()
        w = prods[(z + 8 - sign * (3 - t)) % Z, r, c]
        if t:
            w = w + decoded(short_in[t - 1, r, c])
        short_out[t, r, c] = coded(w)
        go(t_copy(t, u))

    def local_end(u):
        return PARTS[u][0] >= 512 and half_of(u) == 0

    def O(u):
        r, c = spot(u)
        hr, hc = at_home(u)
        own_out[r, c] = coded(prods[z, r, c])
        main_part = PARTS[u][0] < 512
        copy = remote(
            own_out.at[r, c], ends.at[2, core, hr, hc], o_send if main_part else b_send.at[half_of(u)],
            e_recv.at[slot(u), core], home(u, z),
        )
        if local_end(u):
            pl.when(jnp.logical_not(to_self))(copy.start)

            @pl.when(to_self)
            def _():
                ends[2, 1, hr, hc] = own_out[r, c]
        else:
            copy.start()

    def F(u):
        @pl.when(hi == half_of(u))
        def _():
            row, tall, col, wide = PARTS[u]
            hr, hc = at_home(u)
            for c in range(2):
                def arrived(n):
                    bytes_of(ends.at[0, 0, pl.ds(0, n * tall), pl.ds(0, wide)], e_recv.at[slot(u), c])

                if local_end(u) and c == 1:
                    pl.when(to_self)(lambda: arrived(2))
                    pl.when(jnp.logical_not(to_self))(lambda: arrived(3))
                else:
                    arrived(3)
                w = sum(decoded(ends[n, c, hr, hc]) for n in range(3))
                value = w * w * (1.0 / (SCALE * SCALE))
                there = pl.ds(HALF * c + col, wide)
                if row < 512:
                    out_ref[0, pl.ds(row % 256, tall), there] = value
                else:
                    band_ref[0, pl.ds((row - 512) % 64, tall), there] = value

    plan = [
        (sx, 0), (sx, 1), (sx, 2), (st, 0), (sx, 3), (sx, 4), (sx, 5), (ax, 0), (da, 0), (db, 0), (ax, 1), (da, 1),
        (st, 1), (sx, 6), (sx, 7), (sx, 8), (ax, 2), (ax, 3), (re, 0), (db, 1), (da, 2), (ow, 0), (ne, 0), (ax, 4),
        (re, 1), (db, 2), (da, 3), (ax, 5), (ow, 1), (fa, 0), (ne, 1), (ax, 6), (st, 2), (re, 2), (db, 3), (da, 4),
        (pn, 0, 0), (ax, 7), (fa, 1), (ow, 2), (pf, 0, 0), (L, 0, 0), (S, 0, 0), (pn, 1, 0), (O, 0), (ne, 2),
        (ax, 8), (pv,), (pf, 1, 0), (re, 3), (db, 4), (da, 5), (ow, 3), (pa, 0, 1), (L, 1, 0), (S, 1, 0), (fa, 2),
        (L, 0, 1), (S, 0, 1), (L, 0, 2), (S, 0, 2), (pa, 1, 1), (L, 0, 3), (S, 0, 3), (pn, 2), (ne, 3), (pf, 2),
        (L, 0, 4), (S, 0, 4), (L, 0, 5), (S, 0, 5), (O, 1), (O, 2), (O, 3), (O, 4), (O, 5), (re, 4), (db, 5),
        (da, 6), (L, 2, 0), (S, 2, 0), (pn, 3), (L, 1, 1), (fa, 3), (S, 1, 1), (L, 1, 2), (S, 1, 2), (L, 1, 3),
        (S, 1, 3), (ne, 4), (L, 1, 4), (pf, 3), (S, 1, 4), (L, 0, 6), (S, 0, 6), (L, 0, 7), (L, 1, 5), (S, 1, 5),
        (S, 0, 7), (O, 6), (O, 7), (L, 3, 0), (re, 5), (db, 6), (da, 7), (pn, 4), (L, 2, 1), (S, 2, 1), (L, 2, 2),
        (S, 2, 2), (fa, 4), (L, 2, 3), (S, 2, 3), (L, 2, 4), (S, 2, 4), (ne, 5), (L, 1, 6), (pf, 4), (L, 0, 8),
        (S, 0, 8), (L, 0, 9), (S, 1, 6), (L, 1, 7), (S, 0, 9), (O, 8), (O, 9), (re, 6), (db, 7), (da, 8), (L, 2, 5),
        (S, 2, 5), (pn, 5), (L, 3, 1), (L, 3, 2), (S, 1, 7), (fa, 5), (F, 0), (L, 3, 3), (L, 3, 4), (ne, 6),
        (L, 2, 6), (pf, 5), (S, 1, 8), (L, 0, 10), (S, 0, 10), (L, 0, 11), (S, 0, 11), (O, 10), (L, 1, 8), (O, 11),
        (S, 2, 6), (re, 7), (db, 8), (L, 1, 9), (S, 1, 9), (pn, 6), (L, 2, 7), (fa, 6), (L, 3, 5), (S, 2, 7),
        (ne, 7), (F, 1), (S, 2, 8), (pf, 6), (F, 2), (F, 3), (L, 3, 6), (S, 1, 10), (L, 0, 12), (S, 0, 12),
        (L, 0, 13), (S, 0, 13), (F, 4), (O, 12), (O, 13), (re, 8), (S, 1, 11), (L, 1, 10), (pn, 7), (L, 1, 11),
        (fa, 7), (L, 2, 8), (S, 2, 9), (L, 2, 9), (ne, 8), (L, 3, 7), (pf, 7), (L, 0, 14), (S, 0, 14), (L, 0, 15),
        (S, 0, 15), (S, 2, 10), (O, 14), (O, 15), (S, 1, 12), (fa, 8), (F, 5), (pn, 8), (F, 6), (S, 2, 11),
        (L, 1, 12), (L, 1, 13), (S, 1, 13), (pf, 8), (L, 0, 16), (S, 0, 16), (L, 2, 10), (L, 0, 17), (S, 0, 17),
        (pb,), (L, 3, 8), (L, 2, 11), (S, 1, 14), (S, 1, 15), (L, 3, 9), (L, 0, 18), (S, 0, 18), (L, 0, 19),
        (S, 0, 19), (L, 0, 20), (S, 0, 20), (O, 16), (O, 17), (O, 18), (O, 19), (O, 20), (S, 2, 12), (L, 1, 14),
        (F, 7), (L, 0, 21), (S, 0, 21), (O, 21), (S, 2, 13), (L, 1, 15), (L, 2, 12), (S, 1, 16), (L, 2, 13),
        (S, 1, 17), (S, 2, 14), (L, 1, 16), (L, 3, 10), (S, 2, 15), (L, 1, 17), (S, 1, 18), (S, 1, 19), (L, 3, 11),
        (S, 1, 20), (F, 8), (L, 1, 18), (S, 1, 21), (F, 9), (L, 1, 19), (S, 2, 16), (L, 1, 20), (L, 2, 14),
        (S, 2, 17), (L, 1, 21), (L, 2, 15), (L, 3, 12), (S, 2, 18), (L, 3, 13), (S, 2, 19), (L, 2, 16), (S, 2, 20),
        (S, 2, 21), (L, 2, 17), (F, 10), (L, 2, 18), (F, 11), (L, 2, 19), (L, 2, 20), (L, 3, 14), (L, 2, 21),
        (L, 3, 15), (L, 3, 16), (F, 12), (L, 3, 17), (F, 13), (L, 3, 18), (L, 3, 19), (L, 3, 20), (L, 3, 21),
        (F, 14), (F, 15), (F, 16), (F, 17), (F, 18), (F, 19), (F, 20), (F, 21),
    ]
    for step, *at in plan:
        with jax.named_scope("_".join((step.__name__, *map(str, at)))):
            step(*at)

    def close():
        bytes_of(xt, x_send)
        bytes_of(cols.at[pl.ds(0, 4), :, mine], d_send)
        bytes_of(cols.at[pl.ds(0, 2), :, mine], r_send)
        bytes_of(cols.at[:, :, mine], c_send)
        bytes_of(st1.at[pl.ds(0, Z - 1)], s1_send)
        bytes_of(st2, s2_send)
        bytes_of(long_out, l_send)
        bytes_of(short_out, t_send)
        bytes_of(own_out.at[pl.ds(0, 512)], o_send)
        bytes_of(own_out.at[pl.ds(576, 64)], b_send.at[1])
        prev_copy(0).wait_send()
        s3_copy(0).wait_send()

        @pl.when(jnp.logical_not(to_self))
        def _():
            prev_copy(1).wait_send()
            s3_copy(1).wait_send()
            bytes_of(own_out.at[pl.ds(512, 64)], b_send.at[0])

    with jax.named_scope("close"):
        close()


def shards(dosages):
    vmem = pl.BlockSpec(memory_space=pltpu.VMEM)
    dma = pltpu.SemaphoreType.DMA
    n = len(FIRST)
    return pl.pallas_call(
        kernel,
        name="ld",
        out_shape=(
            jax.ShapeDtypeStruct((1, 256, 1024), f32),
            jax.ShapeDtypeStruct((1, 64, 1024), f32),
        ),
        in_specs=[pl.BlockSpec(memory_space=pltpu.HBM)],
        out_specs=(vmem, vmem),
        scratch_shapes=[
            pltpu.VMEM((HALF, 1024), bf16),
            pltpu.VMEM((1024, HALF), bf16),
            pltpu.VMEM((Z, 512, HERE), bf16),
            pltpu.VMEM((HERE, 512), bf16),
            pltpu.VMEM((HERE, 512), bf16),
            pltpu.VMEM((Z, 640, 512), f32),
            pltpu.VMEM((3, 640, 512), bf16),
            pltpu.VMEM((4, 640, 512), bf16),
            pltpu.VMEM((2, 640, 512), bf16),
            pltpu.VMEM((3, 640, 512), bf16),
            pltpu.VMEM((640, 512), bf16),
            pltpu.VMEM((3, 2, 320, 512), bf16),
            pltpu.VMEM((Z, 2, 8, 128), f32),
            pltpu.VMEM((Y, 2, 3, 8, 128), f32),
            pltpu.VMEM((2, 3, 8, 128), f32),
            pltpu.VMEM((Y, 3, 128, 8), f32),
            pltpu.VMEM((2, 3, 1, 512), f32),
            pltpu.VMEM((3, 8, 128), f32),
            dma((4,)),
            dma, dma((n,)), dma((2,)), dma,
            dma, dma, dma, dma, dma((2,)), dma((2,)),
            dma, dma((n, 2)), dma, dma((n,)), dma, dma((n, 3)),
            dma, dma((1 + max(map(max, LONG_AT)),)), dma, dma((1 + max(map(max, SHORT_AT)),)),
            dma, dma((2,)), dma((len(PARTS), 2)),
        ],
        compiler_params=pltpu.CompilerParams(has_side_effects=True, collective_id=0, vmem_limit_bytes=44 * 2**20),
    )(pltpu.with_memory_space_constraint(dosages, pltpu.HBM))


def solution(mesh):
    return jax.shard_map(
        shards,
        mesh=mesh,
        in_specs=(P("samp", ("win", "snp")),),
        out_specs=(P("win", "samp", "snp"), P("win", "samp", "snp")),
        check_vma=False,
    )
```

```python
import jax
import jax.numpy as jnp
from jax import lax
from jax.experimental import pallas as pl
from jax.experimental.pallas import tpu as pltpu
from jax.sharding import PartitionSpec as P

MESH = pl.DeviceIdType.MESH


Z, Y = 8, 4
SAMPLES = 8192
HERE = 1024
HALF = 512
FLOOR = 0.05
POWER = 15
SCALE = 2.0 ** (126.5 / POWER)
FIRST = (0, 64, 128, 192, 256, 320, 384, 448)
ROWS = (64, 64, 64, 64, 64, 64, 64, 64)
PARTS = (
    (0, 64, 0, 256), (0, 64, 256, 256), (64, 64, 0, 256), (64, 64, 256, 256), (128, 32, 0, 512), (160, 32, 0, 512),
    (192, 32, 0, 512), (224, 32, 0, 512), (256, 32, 0, 512), (288, 32, 0, 512), (320, 32, 0, 512),
    (352, 32, 0, 512), (384, 32, 0, 512), (416, 32, 0, 512), (448, 32, 0, 512), (480, 32, 0, 512),
    (576, 32, 0, 512), (608, 32, 0, 512), (512, 32, 0, 512), (544, 32, 0, 512),
)
ENDS = max(sum((r // 256 if r < 512 else (r - 512) // 64) == h for r, _, _, _ in PARTS) for h in range(2))
TURN = sum(row < 128 for row in FIRST)
LONG_AT = (
    (0, 1, 3, 5, 7, 8, 11, 12, 8, 6, 1, 2, 11, 12, 8, 16, 6, 7, 9, 17),
    (2, 4, 0, 1, 2, 3, 5, 9, 3, 10, 14, 15, 18, 1, 10, 13, 4, 11, 12, 14),
    (6, 9, 10, 4, 0, 7, 13, 4, 0, 5, 2, 3, 19, 0, 6, 5, 16, 8, 15, 20),
)
SHORT_AT = (
    (0, 1, 3, 5, 6, 7, 2, 8, 5, 4, 10, 11, 8, 1, 6, 0, 12, 7, 13, 14),
    (2, 4, 0, 1, 3, 9, 0, 6, 7, 2, 9, 3, 4, 5, 10, 11, 2, 15, 9, 1),
)
SIDE_AT = (
    (0, 2, 5, 8, 10, 11, 4, 7),
    (1, 4, 7, 9, 1, 3, 6, 0),
    (3, 6, 0, 2, 5, 8, 10, 11),
)
CORE_AT = (
    (0, 1, 2, 3, 4, 1, 2, 5),
    (0, 6, 1, 3, 1, 3, 1, 3),
    (3, 0, 2, 0, 2, 0, 2, 0),
)

bf16, f32 = jnp.bfloat16, jnp.float32


def coded(w):
    w2 = w * w
    w3 = w2 * w
    w6 = w3 * w3
    w12 = w6 * w6
    return (w12 * w3).astype(bf16)


def decoded(u):
    u = u.astype(f32)
    size = jnp.exp2(jnp.log2(jnp.abs(u)) * (1.0 / POWER))
    return jnp.where(u < 0, -size, size)


def kernel(
    x_hbm, out_ref, band_ref,
    x, xt, cols, own, prev, prods, long_in, long_out, short_in, short_out, own_out, ends,
    st1, st2, st3, rowv, colv, lanes,
    load_sem, x_send, x_recv, p_send, p_recv,
    s1_send, s1_recv, s2_send, s2_recv, s3_send, s3_recv,
    d_send, d_recv, r_send, c_send, c_recv,
    l_send, l_recv, t_send, t_recv, o_send, b_send, e_recv,
):
    samp, win, y = lax.axis_index("samp"), lax.axis_index("win"), lax.axis_index("snp")
    z, hi = samp // 2, samp % 2
    lo, core = win // 2, win % 2

    def dev(z_, hi_, lo_, core_, y_):
        return (2 * z_ + hi_, 2 * lo_ + core_, y_)

    def remote(src, dst, send, recv, to):
        return pltpu.make_async_remote_copy(
            src_ref=src, dst_ref=dst, send_sem=send, recv_sem=recv, device_id=to, device_id_type=MESH
        )

    def go(copy):
        copy.start()

    def bytes_of(ref, sem):
        pltpu.make_async_copy(ref, ref, sem).wait()

    here = dev(z, hi, lo, core, y)
    partner = dev(z, core, 1 - lo, hi, y)
    sibling = dev(z, hi, lo, 1 - core, y)
    up, down = dev(z, hi, lo, core, (y + 1) % Y), dev(z, hi, lo, core, (y + 3) % Y)
    sign = 1 - 2 * core
    fwd, bwd = dev((z + 8 + sign) % Z, hi, lo, core, y), dev((z + 8 - sign) % Z, hi, lo, core, y)
    mine = pl.ds(pl.multiple_of(HALF * core, HALF), HALF)
    by_hi = pl.ds(pl.multiple_of(HALF * hi, HALF), HALF)

    def turn(a):
        xt[pl.ds(128 * a, 128)] = x[:, pl.ds(128 * a, 128)].T

    def load(first, count, k):
        part = pl.ds(128 * first, 128 * count)
        return pltpu.make_async_copy(x_hbm.at[:, part], x.at[:, part], load_sem.at[k])

    loads = [load(0, 1, 0), load(4, 1, 1), load(1, 3, 2), load(5, 3, 3)]
    for copy in loads:
        copy.start()
    barrier = pltpu.get_barrier_semaphore()
    greeted = [dev((z + k) % Z, hi, lo, core, y) for k in range(1, Z)]
    greeted += [dev(z, hi, lo, c, (y + k) % Y) for k in range(1, Y) for c in range(2)]
    greeted += [dev(z, hi ^ (k // 4), lo ^ (k // 2 % 2), core ^ (k % 2), y) for k in range(1, 8)]
    for near in greeted:
        pl.semaphore_signal(barrier, 1, device_id=near, device_id_type=MESH)
    for n in range(2):
        loads[n].wait()
        turn(4 * n)

    pl.semaphore_wait(barrier, len(greeted))

    def rows_of(q):
        return pl.ds(FIRST[q], ROWS[q])

    def x_copy(q, i):
        return remote(
            xt.at[pl.ds(HALF * i + FIRST[q], ROWS[q])], cols.at[2 * y + i, rows_of(q), by_hi],
            x_send, x_recv.at[q], partner,
        )

    def sx(q):
        if q == TURN:
            for a in (1, 5, 2, 6, 3, 7):
                turn(a)
        for i in range(2):
            go(x_copy(q, i))

    next_hi, next_lo = 1 - core, jnp.where(core == 0, 1 - lo, lo)

    def prev_copy(c):
        return remote(
            x.at[:, pl.ds(512 * c, 512)], prev.at[by_hi, :], p_send.at[c], p_recv,
            dev(z, next_hi, next_lo, c, y),
        )

    to_self = jnp.logical_and(hi == 0, core == 1)

    def prev_local():
        return pltpu.make_async_copy(x_hbm.at[:, pl.ds(512, 512)], prev.at[by_hi, :], p_recv)

    def pv():
        go(prev_copy(0))
        pl.when(jnp.logical_not(to_self))(lambda: prev_copy(1).start())
        pl.when(to_self)(lambda: prev_local().start())

    def s1_copy(k):
        return remote(
            st1.at[z], st1.at[z], s1_send, s1_recv, dev((z + k) % Z, hi, lo, core, y)
        )

    def d_copy(q, way, i):
        block = cols.at[2 * y + i, rows_of(q), mine]
        return remote(block, block, d_send, d_recv.at[SIDE_AT[way ^ i][q]], (up, down)[way])

    def r_copy(q, way):
        block = cols.at[2 * ((y + (3, 1)[way]) % Y) + way, rows_of(q), mine]
        return remote(block, block, r_send, d_recv.at[SIDE_AT[2][q]], (up, down)[way])

    def pair(q, k):
        return cols.at[pl.ds(2 * ((y + k) % Y), 2), rows_of(q), mine]

    def c_copy(q, k):
        return remote(pair(q, k), pair(q, k), c_send, c_recv.at[CORE_AT[(0, 1, 2, 1)[k]][q]], sibling)

    def ax(q):
        bytes_of(pair(q, 0), x_recv.at[q])
        go(c_copy(q, 0))

    def da(q):
        for way in range(2):
            go(d_copy(q, way, way))

    def db(q):
        for way in range(2):
            go(d_copy(q, way, 1 - way))

    def re(q):
        bytes_of(pair(q, 0), d_recv.at[SIDE_AT[0][q]])
        for way in range(2):
            go(r_copy(q, way))

    def ne(q):
        bytes_of(pair(q, 0), d_recv.at[SIDE_AT[1][q]])
        for k in (1, 3):
            go(c_copy(q, k))

    def fa(q):
        bytes_of(pair(q, 0), d_recv.at[SIDE_AT[2][q]])
        go(c_copy(q, 2))

    def s2_copy(yy, c):
        return remote(lanes, st2.at[y, hi], s2_send, s2_recv, dev(z, core, 1 - lo, c, yy))

    def s3_copy(c):
        return remote(
            lanes, st3.at[hi], s3_send.at[c], s3_recv.at[hi], dev(z, next_hi, next_lo, c, y)
        )

    def st_sums():
        for n in (2, 3):
            loads[n].wait()

        @pl.loop(0, 8)
        def _(a):
            v = x[:, pl.ds(pl.multiple_of(128 * a, 128), 128)].astype(f32)
            st1[z, 0, pl.ds(a, 1), :] = jnp.sum(v, axis=0, keepdims=True)
            st1[z, 1, pl.ds(a, 1), :] = jnp.sum(v * v, axis=0, keepdims=True)

        for k in range(1, Z):
            go(s1_copy(k))

    def st_send():
        bytes_of(st1.at[pl.ds(0, Z - 1)], s1_recv)
        total = st1[0]
        for k in range(1, Z):
            total = total + st1[k]
        lanes[0] = total[0]
        lanes[1] = total[1]
        lanes[2] = st1[z, 0]
        for c in range(2):
            for k in range(Y):
                go(s2_copy((y + k) % Y, c))
        go(s3_copy(0))
        pl.when(jnp.logical_not(to_self))(lambda: s3_copy(1).start())

        @pl.when(to_self)
        def _():
            st3[hi] = lanes[...]

    def of_sums(parts):
        total, square, local = (parts[k] for k in range(3))
        mean = total * (1.0 / SAMPLES)
        var = jnp.maximum(square * (1.0 / SAMPLES) - mean * mean, FLOOR)
        return mean, 1.0 / jnp.sqrt(var), local

    def st_finish():
        bytes_of(st2, s2_recv)

        for yy in range(Y):
            mean, inv, local = of_sums(st2[yy, 0] + st2[yy, 1])
            e = inv * (SCALE / SAMPLES)
            rowv[yy, 0] = e.T
            rowv[yy, 1] = (local * e).T
            rowv[yy, 2] = (mean * e).T

        def col_vectors(at, parts):
            mean, inv, local = of_sums(parts)
            lanes_of = (inv, mean * inv, (local - HERE * mean) * inv)
            for n, t in enumerate(lanes_of):
                half = jnp.where(core == 0, t[:4], t[4:])
                for j in range(4):
                    colv[at, n, :, pl.ds(128 * j, 128)] = half[j : j + 1]

        col_vectors(0, st2[y, 0] + st2[y, 1])
        for h in range(2):
            there = pltpu.make_async_copy(st3.at[h], st3.at[h], s3_recv.at[h])
            if h == 0:
                pl.when(jnp.logical_not(to_self))(there.wait)
            else:
                there.wait()
        col_vectors(1, st3[0] + st3[1])

    def st(k):
        (st_sums, st_send, st_finish)[k]()

    def ow(m):
        for q in range(len(FIRST)):
            if m == (FIRST[q] + ROWS[q] - 1) // 128:
                c_copy(q, 0).wait_recv()
        own[:, pl.ds(128 * m, 128)] = cols[2 * y + core, pl.ds(128 * m, 128)].T

    def products(left, right, size, yy, tiles, roots, at, inside, to, part):
        g = lax.dot_general(
            left.reshape(2 * size, HERE), right[:, part], (((1,), (0,)), ((), ())), preferred_element_type=f32
        )
        for i in range(2):
            e, s, m = (rowv[yy, n, pl.ds(inside, size), tiles[i] : tiles[i] + 1] for n in range(3))
            v = [colv[at, n, :, part] for n in range(3)]
            prods[roots[i], pl.ds(to, size), part] = g[size * i : size * i + size] * (e * v[0]) - s * v[1] - m * v[2]

    def main(q, ks, n):
        part = pl.ds(0, 512) if n is None else pl.ds(256 * n, 256)
        tile, inside = FIRST[q] // 128, FIRST[q] % 128
        for k in ks:
            yy = (y + k) % Y
            left = cols[pl.ds(2 * yy, 2), rows_of(q)]
            products(left, own, ROWS[q], yy, (tile, 4 + tile), (2 * yy, 2 * yy + 1), 0, inside, FIRST[q], part)

    def pn(q, n=None):
        if not n:
            bytes_of(cols.at[pl.ds(0, 4), rows_of(q), mine], c_recv.at[CORE_AT[1][q]])
        main(q, (0, 1, 3), n)

    def pa(q, n=None):
        main(q, (0, 1, 2, 3), n)

    def pf(q, n=None):
        if not n:
            c_copy(q, 2).wait_recv()
        main(q, (2,), n)

    def pb():
        bytes_of(prev, p_recv)
        for k in range(4):
            left = cols[0:2, pl.ds(128 * k, 128)]
            products(left, prev, 128, 0, (k, 4 + k), (k, 4 + k), 1, 0, 512, pl.ds(0, 512))

    def spot(u):
        row, tall, col, wide = PARTS[u]
        return pl.ds(row, tall), pl.ds(col, wide)

    def half_of(u):
        row = PARTS[u][0]
        return row // 256 if row < 512 else (row - 512) // 64

    def slot(u):
        return sum(half_of(n) == half_of(u) for n in range(u))

    def home(u, z_):
        if PARTS[u][0] < 512:
            return dev(z_, half_of(u), 1 - lo, hi, y)
        return dev(z_, half_of(u), jnp.where(hi == 1, 1 - lo, lo), 1 - hi, y)

    def at_home(u):
        row, tall, col, wide = PARTS[u]
        return pl.ds(row % 256 if row < 512 else 256 + (row - 512) % 64, tall), pl.ds(col, wide)

    def l_copy(t, u):
        r, c = spot(u)
        if t < 3:
            return remote(long_out.at[t, r, c], long_in.at[t, r, c], l_send, l_recv.at[LONG_AT[t][u]], fwd)
        hr, hc = at_home(u)
        return remote(
            long_out.at[t, r, c], ends.at[0, core, hr, hc], l_send, e_recv.at[slot(u), core],
            home(u, (z + 8 + sign) % Z),
        )

    def t_copy(t, u):
        r, c = spot(u)
        if t < 2:
            return remote(short_out.at[t, r, c], short_in.at[t, r, c], t_send, t_recv.at[SHORT_AT[t][u]], bwd)
        hr, hc = at_home(u)
        return remote(
            short_out.at[t, r, c], ends.at[1, core, hr, hc], t_send, e_recv.at[slot(u), core],
            home(u, (z + 8 - sign) % Z),
        )

    def L(t, u):
        r, c = spot(u)
        if t:
            l_copy(t - 1, u).wait_recv()
        w = prods[(z + 8 + sign * (4 - t)) % Z, r, c]
        if t:
            w = w + decoded(long_in[t - 1, r, c])
        long_out[t, r, c] = coded(w)
        go(l_copy(t, u))

    def S(t, u):
        r, c = spot(u)
        if t:
            t_copy(t - 1, u).wait_recv()
        w = prods[(z + 8 - sign * (3 - t)) % Z, r, c]
        if t:
            w = w + decoded(short_in[t - 1, r, c])
        short_out[t, r, c] = coded(w)
        go(t_copy(t, u))

    def local_end(u):
        return PARTS[u][0] >= 512 and half_of(u) == 0

    def O(u):
        r, c = spot(u)
        hr, hc = at_home(u)
        own_out[r, c] = coded(prods[z, r, c])
        main_part = PARTS[u][0] < 512
        copy = remote(
            own_out.at[r, c], ends.at[2, core, hr, hc], o_send if main_part else b_send.at[half_of(u)],
            e_recv.at[slot(u), core], home(u, z),
        )
        if local_end(u):
            pl.when(jnp.logical_not(to_self))(copy.start)

            @pl.when(to_self)
            def _():
                ends[2, 1, hr, hc] = own_out[r, c]
        else:
            copy.start()

    def F(u):
        @pl.when(hi == half_of(u))
        def _():
            row, tall, col, wide = PARTS[u]
            hr, hc = at_home(u)
            for c in range(2):
                def arrived(n):
                    bytes_of(ends.at[0, 0, pl.ds(0, n * tall), pl.ds(0, wide)], e_recv.at[slot(u), c])

                if local_end(u) and c == 1:
                    pl.when(to_self)(lambda: arrived(2))
                    pl.when(jnp.logical_not(to_self))(lambda: arrived(3))
                else:
                    arrived(3)
                w = sum(decoded(ends[n, c, hr, hc]) for n in range(3))
                value = w * w * (1.0 / (SCALE * SCALE))
                there = pl.ds(HALF * c + col, wide)
                if row < 512:
                    out_ref[0, pl.ds(row % 256, tall), there] = value
                else:
                    band_ref[0, pl.ds((row - 512) % 64, tall), there] = value

    plan = [
        (sx, 0), (sx, 1), (st, 0), (sx, 2), (sx, 3), (sx, 4), (sx, 5), (ax, 0), (da, 0), (db, 0), (st, 1), (sx, 6),
        (sx, 7), (ax, 1), (da, 1), (ax, 2), (ow, 0), (ax, 3), (re, 0), (db, 1), (da, 2), (ax, 4), (ow, 1), (ne, 0),
        (ax, 5), (re, 1), (db, 2), (da, 3), (ow, 2), (ax, 6), (fa, 0), (st, 2), (pn, 0, 0), (ax, 7), (pv,), (ne, 1),
        (pf, 0, 0), (L, 0, 0), (S, 0, 0), (O, 0), (re, 2), (db, 3), (da, 4), (ow, 3), (pa, 0, 1), (L, 0, 1),
        (S, 0, 1), (pn, 1, 0), (fa, 1), (O, 1), (ne, 2), (L, 1, 0), (S, 1, 0), (pf, 1, 0), (L, 0, 2), (S, 0, 2),
        (pa, 1, 1), (re, 3), (db, 4), (da, 5), (L, 1, 1), (S, 1, 1), (L, 0, 3), (S, 0, 3), (O, 2), (O, 3), (pn, 2),
        (fa, 2), (L, 2, 0), (S, 2, 0), (ne, 3), (L, 1, 2), (S, 1, 2), (pf, 2), (L, 0, 4), (S, 0, 4), (L, 0, 5),
        (L, 2, 1), (S, 2, 1), (S, 0, 5), (O, 4), (O, 5), (re, 4), (db, 5), (da, 6), (L, 1, 3), (S, 1, 3), (pn, 3),
        (fa, 3), (L, 3, 0), (L, 2, 2), (S, 2, 2), (ne, 4), (L, 1, 4), (S, 1, 4), (pf, 3), (L, 1, 5), (L, 0, 6),
        (S, 0, 6), (L, 0, 7), (S, 0, 7), (O, 6), (O, 7), (re, 5), (db, 6), (da, 7), (L, 3, 1), (S, 1, 5), (pn, 4),
        (fa, 4), (L, 2, 3), (S, 2, 3), (L, 3, 2), (S, 2, 4), (ne, 5), (F, 0), (L, 2, 4), (S, 1, 6), (pf, 4),
        (L, 0, 8), (S, 0, 8), (L, 0, 9), (L, 2, 5), (S, 1, 7), (S, 0, 9), (O, 8), (O, 9), (re, 6), (db, 7),
        (L, 1, 6), (S, 2, 5), (pn, 5), (fa, 5), (L, 1, 7), (L, 3, 3), (S, 2, 6), (ne, 6), (F, 1), (pf, 5), (S, 1, 8),
        (L, 0, 10), (S, 0, 10), (L, 0, 11), (S, 0, 11), (L, 3, 4), (O, 10), (S, 2, 7), (re, 7), (O, 11), (F, 2),
        (L, 1, 8), (S, 1, 9), (pn, 6), (fa, 6), (L, 1, 9), (L, 3, 5), (L, 2, 6), (ne, 7), (S, 2, 8), (L, 2, 7),
        (pf, 6), (S, 1, 10), (L, 0, 12), (S, 0, 12), (L, 0, 13), (S, 0, 13), (O, 12), (O, 13), (S, 1, 11),
        (L, 1, 10), (fa, 7), (pn, 7), (F, 3), (L, 1, 11), (S, 2, 9), (pf, 7), (L, 2, 8), (L, 0, 14), (S, 0, 14),
        (L, 0, 15), (F, 4), (S, 2, 10), (S, 0, 15), (pb,), (L, 3, 6), (L, 2, 9), (S, 1, 12), (S, 1, 13), (L, 0, 16),
        (S, 0, 16), (F, 5), (S, 2, 11), (L, 3, 7), (L, 0, 17), (S, 0, 17), (L, 0, 18), (S, 0, 18), (L, 0, 19),
        (S, 0, 19), (O, 14), (O, 15), (O, 16), (O, 17), (O, 18), (O, 19), (L, 1, 12), (S, 1, 14), (L, 1, 13),
        (L, 2, 10), (S, 1, 15), (L, 2, 11), (S, 2, 12), (L, 3, 8), (S, 2, 13), (L, 1, 14), (S, 1, 16), (L, 1, 15),
        (S, 1, 17), (L, 3, 9), (F, 6), (S, 1, 18), (L, 1, 16), (S, 1, 19), (S, 2, 14), (L, 1, 17), (F, 7),
        (S, 2, 15), (L, 1, 18), (L, 1, 19), (L, 2, 12), (S, 2, 16), (L, 2, 13), (S, 2, 17), (L, 3, 10), (S, 2, 18),
        (L, 3, 11), (S, 2, 19), (L, 2, 14), (F, 8), (L, 2, 15), (L, 2, 16), (F, 9), (L, 2, 17), (L, 2, 18),
        (L, 2, 19), (L, 3, 12), (L, 3, 13), (L, 3, 14), (L, 3, 15), (F, 10), (F, 11), (L, 3, 16), (L, 3, 17),
        (L, 3, 18), (L, 3, 19), (F, 12), (F, 13), (F, 14), (F, 15), (F, 16), (F, 17), (F, 18), (F, 19),
    ]
    for step, *at in plan:
        with jax.named_scope("_".join((step.__name__, *map(str, at)))):
            step(*at)

    def close():
        bytes_of(xt, x_send)
        bytes_of(cols.at[pl.ds(0, 4), :, mine], d_send)
        bytes_of(cols.at[pl.ds(0, 2), :, mine], r_send)
        bytes_of(cols.at[:, :, mine], c_send)
        bytes_of(st1.at[pl.ds(0, Z - 1)], s1_send)
        bytes_of(st2, s2_send)
        bytes_of(long_out, l_send)
        bytes_of(short_out, t_send)
        bytes_of(own_out.at[pl.ds(0, 512)], o_send)
        bytes_of(own_out.at[pl.ds(576, 64)], b_send.at[1])
        prev_copy(0).wait_send()
        s3_copy(0).wait_send()

        @pl.when(jnp.logical_not(to_self))
        def _():
            prev_copy(1).wait_send()
            s3_copy(1).wait_send()
            bytes_of(own_out.at[pl.ds(512, 64)], b_send.at[0])

    with jax.named_scope("close"):
        close()


def shards(dosages):
    vmem = pl.BlockSpec(memory_space=pltpu.VMEM)
    dma = pltpu.SemaphoreType.DMA
    n = len(FIRST)
    return pl.pallas_call(
        kernel,
        name="ld",
        out_shape=(
            jax.ShapeDtypeStruct((1, 256, 1024), f32),
            jax.ShapeDtypeStruct((1, 64, 1024), f32),
        ),
        in_specs=[pl.BlockSpec(memory_space=pltpu.HBM)],
        out_specs=(vmem, vmem),
        scratch_shapes=[
            pltpu.VMEM((HALF, 1024), bf16),
            pltpu.VMEM((1024, HALF), bf16),
            pltpu.VMEM((Z, 512, HERE), bf16),
            pltpu.VMEM((HERE, 512), bf16),
            pltpu.VMEM((HERE, 512), bf16),
            pltpu.VMEM((Z, 640, 512), f32),
            pltpu.VMEM((3, 640, 512), bf16),
            pltpu.VMEM((4, 640, 512), bf16),
            pltpu.VMEM((2, 640, 512), bf16),
            pltpu.VMEM((3, 640, 512), bf16),
            pltpu.VMEM((640, 512), bf16),
            pltpu.VMEM((3, 2, 320, 512), bf16),
            pltpu.VMEM((Z, 2, 8, 128), f32),
            pltpu.VMEM((Y, 2, 3, 8, 128), f32),
            pltpu.VMEM((2, 3, 8, 128), f32),
            pltpu.VMEM((Y, 3, 128, 8), f32),
            pltpu.VMEM((2, 3, 1, 512), f32),
            pltpu.VMEM((3, 8, 128), f32),
            dma((4,)),
            dma, dma((n,)), dma((2,)), dma,
            dma, dma, dma, dma, dma((2,)), dma((2,)),
            dma, dma((1 + max(map(max, SIDE_AT)),)), dma, dma, dma((1 + max(map(max, CORE_AT)),)),
            dma, dma((1 + max(map(max, LONG_AT)),)), dma, dma((1 + max(map(max, SHORT_AT)),)),
            dma, dma((2,)), dma((ENDS, 2)),
        ],
        compiler_params=pltpu.CompilerParams(has_side_effects=True, collective_id=0, vmem_limit_bytes=44 * 2**20),
    )(pltpu.with_memory_space_constraint(dosages, pltpu.HBM))


def solution(mesh):
    return jax.shard_map(
        shards,
        mesh=mesh,
        in_specs=(P("samp", ("win", "snp")),),
        out_specs=(P("win", "samp", "snp"), P("win", "samp", "snp")),
        check_vma=False,
    )
```

```python
import jax
import jax.numpy as jnp
from jax import lax
from jax.experimental import pallas as pl
from jax.experimental.pallas import tpu as pltpu
from jax.sharding import PartitionSpec as P

MESH = pl.DeviceIdType.MESH


Z, Y = 8, 4
SAMPLES = 8192
HERE = 1024
HALF = 512
FLOOR = 0.05
POWER = 15
SCALE = 2.0 ** (126.5 / POWER)
FIRST = (0, 32, 64, 128, 192, 256, 320, 384, 448)
ROWS = (32, 32, 64, 64, 64, 64, 64, 64, 64)
PARTS = (
    (0, 32, 0, 256), (0, 32, 256, 256), (32, 32, 0, 256), (32, 32, 256, 256), (64, 64, 0, 256), (64, 64, 256, 256),
    (128, 32, 0, 512), (160, 32, 0, 512), (192, 32, 0, 512), (224, 32, 0, 512), (256, 32, 0, 512),
    (288, 32, 0, 512), (320, 32, 0, 512), (352, 32, 0, 512), (384, 32, 0, 512), (416, 32, 0, 512),
    (448, 32, 0, 512), (480, 32, 0, 512), (576, 32, 0, 512), (608, 32, 0, 512), (512, 32, 0, 512),
    (544, 32, 0, 512),
)
ENDS = max(sum((r // 256 if r < 512 else (r - 512) // 64) == h for r, _, _, _ in PARTS) for h in range(2))
TURN = sum(row < 128 for row in FIRST)
LONG_AT = (
    (0, 2, 3, 4, 5, 6, 12, 13, 2, 15, 8, 9, 1, 3, 15, 16, 7, 17, 8, 9, 10, 1),
    (1, 0, 8, 9, 10, 11, 6, 16, 10, 11, 4, 5, 14, 0, 11, 13, 5, 2, 6, 4, 15, 0),
    (7, 14, 1, 3, 4, 5, 0, 13, 6, 2, 12, 18, 19, 3, 14, 16, 18, 8, 9, 7, 12, 17),
)
SHORT_AT = (
    (0, 2, 3, 4, 5, 6, 11, 12, 5, 4, 10, 9, 0, 2, 5, 12, 9, 8, 10, 1, 13, 0),
    (1, 0, 7, 8, 9, 10, 6, 3, 8, 11, 7, 6, 3, 4, 11, 14, 7, 2, 6, 15, 16, 3),
)
SIDE_AT = (
    (0, 2, 4, 8, 11, 1, 12, 6, 10),
    (1, 3, 7, 10, 0, 3, 5, 9, 0),
    (5, 6, 9, 2, 4, 8, 11, 1, 12),
)
CORE_AT = (
    (0, 1, 2, 3, 4, 0, 2, 8, 6),
    (5, 6, 5, 0, 6, 7, 6, 7, 6),
    (1, 7, 7, 5, 0, 5, 0, 5, 0),
)

bf16, f32 = jnp.bfloat16, jnp.float32


def coded(w):
    w2 = w * w
    w3 = w2 * w
    w6 = w3 * w3
    w12 = w6 * w6
    return (w12 * w3).astype(bf16)


def decoded(u):
    u = u.astype(f32)
    size = jnp.exp2(jnp.log2(jnp.abs(u)) * (1.0 / POWER))
    return jnp.where(u < 0, -size, size)


def kernel(
    x_hbm, out_ref, band_ref,
    x, xt, cols, own, prev, prods, long_in, long_out, short_in, short_out, own_out, ends,
    st1, st2, st3, rowv, colv, lanes,
    load_sem, x_send, x_recv, p_send, p_recv,
    s1_send, s1_recv, s2_send, s2_recv, s3_send, s3_recv,
    d_send, d_recv, r_send, c_send, c_recv,
    l_send, l_recv, t_send, t_recv, o_send, b_send, e_recv,
):
    samp, win, y = lax.axis_index("samp"), lax.axis_index("win"), lax.axis_index("snp")
    z, hi = samp // 2, samp % 2
    lo, core = win // 2, win % 2

    def dev(z_, hi_, lo_, core_, y_):
        return (2 * z_ + hi_, 2 * lo_ + core_, y_)

    def remote(src, dst, send, recv, to):
        return pltpu.make_async_remote_copy(
            src_ref=src, dst_ref=dst, send_sem=send, recv_sem=recv, device_id=to, device_id_type=MESH
        )

    def go(copy):
        copy.start()

    def bytes_of(ref, sem):
        pltpu.make_async_copy(ref, ref, sem).wait()

    here = dev(z, hi, lo, core, y)
    partner = dev(z, core, 1 - lo, hi, y)
    sibling = dev(z, hi, lo, 1 - core, y)
    up, down = dev(z, hi, lo, core, (y + 1) % Y), dev(z, hi, lo, core, (y + 3) % Y)
    sign = 1 - 2 * core
    fwd, bwd = dev((z + 8 + sign) % Z, hi, lo, core, y), dev((z + 8 - sign) % Z, hi, lo, core, y)
    mine = pl.ds(pl.multiple_of(HALF * core, HALF), HALF)
    by_hi = pl.ds(pl.multiple_of(HALF * hi, HALF), HALF)

    def turn(a):
        xt[pl.ds(128 * a, 128)] = x[:, pl.ds(128 * a, 128)].T

    def load(first, count, k):
        part = pl.ds(128 * first, 128 * count)
        return pltpu.make_async_copy(x_hbm.at[:, part], x.at[:, part], load_sem.at[k])

    loads = [load(0, 1, 0), load(4, 1, 1), load(1, 3, 2), load(5, 3, 3)]
    for copy in loads:
        copy.start()
    barrier = pltpu.get_barrier_semaphore()
    greeted = [dev((z + k) % Z, hi, lo, core, y) for k in range(1, Z)]
    greeted += [dev(z, hi, lo, c, (y + k) % Y) for k in range(1, Y) for c in range(2)]
    greeted += [dev(z, hi ^ (k // 4), lo ^ (k // 2 % 2), core ^ (k % 2), y) for k in range(1, 8)]
    for near in greeted:
        pl.semaphore_signal(barrier, 1, device_id=near, device_id_type=MESH)
    for n in range(2):
        loads[n].wait()
        turn(4 * n)

    pl.semaphore_wait(barrier, len(greeted))

    def rows_of(q):
        return pl.ds(FIRST[q], ROWS[q])

    def x_copy(q, i):
        return remote(
            xt.at[pl.ds(HALF * i + FIRST[q], ROWS[q])], cols.at[2 * y + i, rows_of(q), by_hi],
            x_send, x_recv.at[q], partner,
        )

    def sx(q):
        if q == TURN:
            for a in (1, 5, 2, 6, 3, 7):
                turn(a)
        for i in range(2):
            go(x_copy(q, i))

    next_hi, next_lo = 1 - core, jnp.where(core == 0, 1 - lo, lo)

    def prev_copy(c):
        return remote(
            x.at[:, pl.ds(512 * c, 512)], prev.at[by_hi, :], p_send.at[c], p_recv,
            dev(z, next_hi, next_lo, c, y),
        )

    to_self = jnp.logical_and(hi == 0, core == 1)

    def prev_local():
        return pltpu.make_async_copy(x_hbm.at[:, pl.ds(512, 512)], prev.at[by_hi, :], p_recv)

    def pv():
        go(prev_copy(0))
        pl.when(jnp.logical_not(to_self))(lambda: prev_copy(1).start())
        pl.when(to_self)(lambda: prev_local().start())

    def s1_copy(k):
        return remote(
            st1.at[z], st1.at[z], s1_send, s1_recv, dev((z + k) % Z, hi, lo, core, y)
        )

    def d_copy(q, way, i):
        block = cols.at[2 * y + i, rows_of(q), mine]
        return remote(block, block, d_send, d_recv.at[SIDE_AT[way ^ i][q]], (up, down)[way])

    def r_copy(q, way):
        block = cols.at[2 * ((y + (3, 1)[way]) % Y) + way, rows_of(q), mine]
        return remote(block, block, r_send, d_recv.at[SIDE_AT[2][q]], (up, down)[way])

    def pair(q, k):
        return cols.at[pl.ds(2 * ((y + k) % Y), 2), rows_of(q), mine]

    def c_copy(q, k):
        return remote(pair(q, k), pair(q, k), c_send, c_recv.at[CORE_AT[(0, 1, 2, 1)[k]][q]], sibling)

    def ax(q):
        bytes_of(pair(q, 0), x_recv.at[q])
        go(c_copy(q, 0))

    def da(q):
        for way in range(2):
            go(d_copy(q, way, way))

    def db(q):
        for way in range(2):
            go(d_copy(q, way, 1 - way))

    def re(q):
        bytes_of(pair(q, 0), d_recv.at[SIDE_AT[0][q]])
        for way in range(2):
            go(r_copy(q, way))

    def ne(q):
        bytes_of(pair(q, 0), d_recv.at[SIDE_AT[1][q]])
        for k in (1, 3):
            go(c_copy(q, k))

    def fa(q):
        bytes_of(pair(q, 0), d_recv.at[SIDE_AT[2][q]])
        go(c_copy(q, 2))

    def s2_copy(yy, c):
        return remote(lanes, st2.at[y, hi], s2_send, s2_recv, dev(z, core, 1 - lo, c, yy))

    def s3_copy(c):
        return remote(
            lanes, st3.at[hi], s3_send.at[c], s3_recv.at[hi], dev(z, next_hi, next_lo, c, y)
        )

    def st_sums():
        for n in (2, 3):
            loads[n].wait()

        @pl.loop(0, 8)
        def _(a):
            v = x[:, pl.ds(pl.multiple_of(128 * a, 128), 128)].astype(f32)
            st1[z, 0, pl.ds(a, 1), :] = jnp.sum(v, axis=0, keepdims=True)
            st1[z, 1, pl.ds(a, 1), :] = jnp.sum(v * v, axis=0, keepdims=True)

        for k in range(1, Z):
            go(s1_copy(k))

    def st_send():
        bytes_of(st1.at[pl.ds(0, Z - 1)], s1_recv)
        total = st1[0]
        for k in range(1, Z):
            total = total + st1[k]
        lanes[0] = total[0]
        lanes[1] = total[1]
        lanes[2] = st1[z, 0]
        for c in range(2):
            for k in range(Y):
                go(s2_copy((y + k) % Y, c))
        go(s3_copy(0))
        pl.when(jnp.logical_not(to_self))(lambda: s3_copy(1).start())

        @pl.when(to_self)
        def _():
            st3[hi] = lanes[...]

    def of_sums(parts):
        total, square, local = (parts[k] for k in range(3))
        mean = total * (1.0 / SAMPLES)
        var = jnp.maximum(square * (1.0 / SAMPLES) - mean * mean, FLOOR)
        return mean, 1.0 / jnp.sqrt(var), local

    def st_finish():
        bytes_of(st2, s2_recv)

        for yy in range(Y):
            mean, inv, local = of_sums(st2[yy, 0] + st2[yy, 1])
            e = inv * (SCALE / SAMPLES)
            rowv[yy, 0] = e.T
            rowv[yy, 1] = (local * e).T
            rowv[yy, 2] = (mean * e).T

        def col_vectors(at, parts):
            mean, inv, local = of_sums(parts)
            lanes_of = (inv, mean * inv, (local - HERE * mean) * inv)
            for n, t in enumerate(lanes_of):
                half = jnp.where(core == 0, t[:4], t[4:])
                for j in range(4):
                    colv[at, n, :, pl.ds(128 * j, 128)] = half[j : j + 1]

        col_vectors(0, st2[y, 0] + st2[y, 1])
        for h in range(2):
            there = pltpu.make_async_copy(st3.at[h], st3.at[h], s3_recv.at[h])
            if h == 0:
                pl.when(jnp.logical_not(to_self))(there.wait)
            else:
                there.wait()
        col_vectors(1, st3[0] + st3[1])

    def st(k):
        (st_sums, st_send, st_finish)[k]()

    def ow(m):
        for q in range(len(FIRST)):
            if m == (FIRST[q] + ROWS[q] - 1) // 128:
                c_copy(q, 0).wait_recv()
        own[:, pl.ds(128 * m, 128)] = cols[2 * y + core, pl.ds(128 * m, 128)].T

    def products(left, right, size, yy, tiles, roots, at, inside, to, part):
        g = lax.dot_general(
            left.reshape(2 * size, HERE), right[:, part], (((1,), (0,)), ((), ())), preferred_element_type=f32
        )
        for i in range(2):
            e, s, m = (rowv[yy, n, pl.ds(inside, size), tiles[i] : tiles[i] + 1] for n in range(3))
            v = [colv[at, n, :, part] for n in range(3)]
            prods[roots[i], pl.ds(to, size), part] = g[size * i : size * i + size] * (e * v[0]) - s * v[1] - m * v[2]

    def main(q, ks, n):
        part = pl.ds(0, 512) if n is None else pl.ds(256 * n, 256)
        tile, inside = FIRST[q] // 128, FIRST[q] % 128
        for k in ks:
            yy = (y + k) % Y
            left = cols[pl.ds(2 * yy, 2), rows_of(q)]
            products(left, own, ROWS[q], yy, (tile, 4 + tile), (2 * yy, 2 * yy + 1), 0, inside, FIRST[q], part)

    def pn(q, n=None):
        if not n:
            bytes_of(cols.at[pl.ds(0, 4), rows_of(q), mine], c_recv.at[CORE_AT[1][q]])
        main(q, (0, 1, 3), n)

    def pa(q, n=None):
        main(q, (0, 1, 2, 3), n)

    def pf(q, n=None):
        if not n:
            c_copy(q, 2).wait_recv()
        main(q, (2,), n)

    def pb():
        bytes_of(prev, p_recv)
        for k in range(4):
            left = cols[0:2, pl.ds(128 * k, 128)]
            products(left, prev, 128, 0, (k, 4 + k), (k, 4 + k), 1, 0, 512, pl.ds(0, 512))

    def spot(u):
        row, tall, col, wide = PARTS[u]
        return pl.ds(row, tall), pl.ds(col, wide)

    def half_of(u):
        row = PARTS[u][0]
        return row // 256 if row < 512 else (row - 512) // 64

    def slot(u):
        return sum(half_of(n) == half_of(u) for n in range(u))

    def home(u, z_):
        if PARTS[u][0] < 512:
            return dev(z_, half_of(u), 1 - lo, hi, y)
        return dev(z_, half_of(u), jnp.where(hi == 1, 1 - lo, lo), 1 - hi, y)

    def at_home(u):
        row, tall, col, wide = PARTS[u]
        return pl.ds(row % 256 if row < 512 else 256 + (row - 512) % 64, tall), pl.ds(col, wide)

    def l_copy(t, u):
        r, c = spot(u)
        if t < 3:
            return remote(long_out.at[t, r, c], long_in.at[t, r, c], l_send, l_recv.at[LONG_AT[t][u]], fwd)
        hr, hc = at_home(u)
        return remote(
            long_out.at[t, r, c], ends.at[0, core, hr, hc], l_send, e_recv.at[slot(u), core],
            home(u, (z + 8 + sign) % Z),
        )

    def t_copy(t, u):
        r, c = spot(u)
        if t < 2:
            return remote(short_out.at[t, r, c], short_in.at[t, r, c], t_send, t_recv.at[SHORT_AT[t][u]], bwd)
        hr, hc = at_home(u)
        return remote(
            short_out.at[t, r, c], ends.at[1, core, hr, hc], t_send, e_recv.at[slot(u), core],
            home(u, (z + 8 - sign) % Z),
        )

    def L(t, u):
        r, c = spot(u)
        if t:
            l_copy(t - 1, u).wait_recv()
        w = prods[(z + 8 + sign * (4 - t)) % Z, r, c]
        if t:
            w = w + decoded(long_in[t - 1, r, c])
        long_out[t, r, c] = coded(w)
        go(l_copy(t, u))

    def S(t, u):
        r, c = spot(u)
        if t:
            t_copy(t - 1, u).wait_recv()
        w = prods[(z + 8 - sign * (3 - t)) % Z, r, c]
        if t:
            w = w + decoded(short_in[t - 1, r, c])
        short_out[t, r, c] = coded(w)
        go(t_copy(t, u))

    def local_end(u):
        return PARTS[u][0] >= 512 and half_of(u) == 0

    def O(u):
        r, c = spot(u)
        hr, hc = at_home(u)
        own_out[r, c] = coded(prods[z, r, c])
        main_part = PARTS[u][0] < 512
        copy = remote(
            own_out.at[r, c], ends.at[2, core, hr, hc], o_send if main_part else b_send.at[half_of(u)],
            e_recv.at[slot(u), core], home(u, z),
        )
        if local_end(u):
            pl.when(jnp.logical_not(to_self))(copy.start)

            @pl.when(to_self)
            def _():
                ends[2, 1, hr, hc] = own_out[r, c]
        else:
            copy.start()

    def F(u):
        @pl.when(hi == half_of(u))
        def _():
            row, tall, col, wide = PARTS[u]
            hr, hc = at_home(u)
            for c in range(2):
                def arrived(n):
                    bytes_of(ends.at[0, 0, pl.ds(0, n * tall), pl.ds(0, wide)], e_recv.at[slot(u), c])

                if local_end(u) and c == 1:
                    pl.when(to_self)(lambda: arrived(2))
                    pl.when(jnp.logical_not(to_self))(lambda: arrived(3))
                else:
                    arrived(3)
                w = sum(decoded(ends[n, c, hr, hc]) for n in range(3))
                value = w * w * (1.0 / (SCALE * SCALE))
                there = pl.ds(HALF * c + col, wide)
                if row < 512:
                    out_ref[0, pl.ds(row % 256, tall), there] = value
                else:
                    band_ref[0, pl.ds((row - 512) % 64, tall), there] = value

    plan = [
        (sx, 0), (sx, 1), (sx, 2), (st, 0), (sx, 3), (sx, 4), (ax, 0), (da, 0), (db, 0), (ax, 1), (da, 1), (db, 1),
        (st, 1), (sx, 5), (sx, 6), (sx, 7), (sx, 8), (ax, 2), (da, 2), (ax, 3), (ow, 0), (re, 0), (ax, 4), (ne, 0),
        (re, 1), (db, 2), (da, 3), (ne, 1), (ow, 1), (ax, 5), (st, 2), (re, 2), (db, 3), (da, 4), (fa, 0),
        (pn, 0, 0), (ax, 6), (pn, 1, 0), (fa, 1), (ax, 7), (pf, 0, 0), (L, 0, 0), (S, 0, 0), (O, 0), (ow, 2),
        (ne, 2), (pf, 1, 0), (ax, 8), (pv,), (re, 3), (db, 4), (da, 5), (pn, 2, 0), (ow, 3), (L, 1, 0), (fa, 2),
        (S, 1, 0), (pa, 0, 1), (L, 0, 1), (S, 0, 1), (L, 0, 2), (S, 0, 2), (pa, 1, 1), (L, 0, 3), (ne, 3), (S, 0, 3),
        (O, 1), (O, 2), (O, 3), (pf, 2, 0), (L, 0, 4), (S, 0, 4), (pa, 2, 1), (re, 4), (db, 5), (da, 6), (L, 0, 5),
        (S, 0, 5), (L, 2, 0), (S, 2, 0), (O, 4), (O, 5), (pn, 3), (fa, 3), (L, 1, 1), (S, 1, 1), (L, 1, 2),
        (S, 1, 2), (L, 1, 3), (S, 1, 3), (ne, 4), (L, 1, 4), (S, 1, 4), (pf, 3), (L, 1, 5), (S, 1, 5), (L, 0, 6),
        (S, 0, 6), (L, 0, 7), (L, 3, 0), (S, 0, 7), (O, 6), (O, 7), (re, 5), (db, 6), (da, 7), (L, 2, 1), (S, 2, 1),
        (L, 2, 2), (pn, 4), (fa, 4), (S, 2, 2), (L, 2, 3), (S, 2, 3), (L, 2, 4), (S, 2, 4), (ne, 5), (L, 2, 5),
        (S, 2, 5), (pf, 4), (L, 1, 6), (S, 1, 6), (L, 0, 8), (S, 0, 8), (L, 0, 9), (S, 0, 9), (O, 8), (O, 9),
        (re, 6), (db, 7), (da, 8), (L, 1, 7), (S, 1, 7), (pn, 5), (fa, 5), (L, 3, 1), (L, 3, 2), (L, 3, 3), (F, 0),
        (L, 3, 4), (ne, 6), (L, 3, 5), (pf, 5), (S, 2, 6), (L, 2, 6), (L, 0, 10), (S, 0, 10), (L, 0, 11), (S, 0, 11),
        (O, 10), (O, 11), (re, 7), (db, 8), (S, 1, 8), (L, 1, 8), (pn, 6), (fa, 6), (L, 1, 9), (S, 2, 7), (L, 2, 7),
        (S, 1, 9), (ne, 7), (F, 1), (F, 2), (F, 3), (pf, 6), (S, 1, 10), (L, 0, 12), (S, 0, 12), (L, 0, 13), (F, 4),
        (S, 0, 13), (re, 8), (L, 3, 6), (O, 12), (S, 1, 11), (O, 13), (F, 5), (L, 1, 10), (pn, 7), (fa, 7),
        (S, 2, 8), (L, 1, 11), (L, 2, 8), (S, 2, 9), (ne, 8), (L, 2, 9), (S, 2, 10), (pf, 7), (L, 3, 7), (S, 1, 12),
        (L, 0, 14), (S, 0, 14), (L, 0, 15), (S, 0, 15), (O, 14), (O, 15), (L, 1, 12), (S, 1, 13), (fa, 8), (pn, 8),
        (S, 2, 11), (L, 1, 13), (L, 2, 10), (pf, 8), (F, 6), (L, 0, 16), (S, 0, 16), (L, 0, 17), (L, 2, 11),
        (S, 0, 17), (pb,), (L, 3, 8), (L, 3, 9), (S, 2, 12), (S, 1, 14), (L, 0, 18), (S, 0, 18), (L, 0, 19),
        (S, 0, 19), (L, 0, 20), (S, 0, 20), (S, 1, 15), (O, 16), (O, 17), (O, 18), (O, 19), (O, 20), (L, 1, 14),
        (S, 2, 13), (F, 7), (L, 0, 21), (S, 0, 21), (O, 21), (L, 1, 15), (L, 2, 12), (S, 1, 16), (L, 2, 13),
        (S, 1, 17), (L, 3, 10), (L, 1, 16), (S, 2, 14), (L, 1, 17), (S, 1, 18), (L, 3, 11), (S, 1, 19), (S, 1, 20),
        (S, 2, 15), (F, 8), (L, 1, 18), (F, 9), (L, 1, 19), (S, 1, 21), (L, 1, 20), (S, 2, 16), (L, 2, 14),
        (S, 2, 17), (L, 1, 21), (L, 2, 15), (S, 2, 18), (L, 3, 12), (S, 2, 19), (L, 3, 13), (S, 2, 20), (L, 2, 16),
        (S, 2, 21), (F, 10), (L, 2, 17), (L, 2, 18), (F, 11), (L, 2, 19), (L, 2, 20), (L, 3, 14), (L, 2, 21),
        (L, 3, 15), (L, 3, 16), (L, 3, 17), (F, 12), (L, 3, 18), (F, 13), (L, 3, 19), (L, 3, 20), (L, 3, 21),
        (F, 14), (F, 15), (F, 16), (F, 17), (F, 18), (F, 19), (F, 20), (F, 21),
    ]
    for step, *at in plan:
        with jax.named_scope("_".join((step.__name__, *map(str, at)))):
            step(*at)

    def close():
        bytes_of(xt, x_send)
        bytes_of(cols.at[pl.ds(0, 4), :, mine], d_send)
        bytes_of(cols.at[pl.ds(0, 2), :, mine], r_send)
        bytes_of(cols.at[:, :, mine], c_send)
        bytes_of(st1.at[pl.ds(0, Z - 1)], s1_send)
        bytes_of(st2, s2_send)
        bytes_of(long_out, l_send)
        bytes_of(short_out, t_send)
        bytes_of(own_out.at[pl.ds(0, 512)], o_send)
        bytes_of(own_out.at[pl.ds(576, 64)], b_send.at[1])
        prev_copy(0).wait_send()
        s3_copy(0).wait_send()

        @pl.when(jnp.logical_not(to_self))
        def _():
            prev_copy(1).wait_send()
            s3_copy(1).wait_send()
            bytes_of(own_out.at[pl.ds(512, 64)], b_send.at[0])

    with jax.named_scope("close"):
        close()


def shards(dosages):
    vmem = pl.BlockSpec(memory_space=pltpu.VMEM)
    dma = pltpu.SemaphoreType.DMA
    n = len(FIRST)
    return pl.pallas_call(
        kernel,
        name="ld",
        out_shape=(
            jax.ShapeDtypeStruct((1, 256, 1024), f32),
            jax.ShapeDtypeStruct((1, 64, 1024), f32),
        ),
        in_specs=[pl.BlockSpec(memory_space=pltpu.HBM)],
        out_specs=(vmem, vmem),
        scratch_shapes=[
            pltpu.VMEM((HALF, 1024), bf16),
            pltpu.VMEM((1024, HALF), bf16),
            pltpu.VMEM((Z, 512, HERE), bf16),
            pltpu.VMEM((HERE, 512), bf16),
            pltpu.VMEM((HERE, 512), bf16),
            pltpu.VMEM((Z, 640, 512), f32),
            pltpu.VMEM((3, 640, 512), bf16),
            pltpu.VMEM((4, 640, 512), bf16),
            pltpu.VMEM((2, 640, 512), bf16),
            pltpu.VMEM((3, 640, 512), bf16),
            pltpu.VMEM((640, 512), bf16),
            pltpu.VMEM((3, 2, 320, 512), bf16),
            pltpu.VMEM((Z, 2, 8, 128), f32),
            pltpu.VMEM((Y, 2, 3, 8, 128), f32),
            pltpu.VMEM((2, 3, 8, 128), f32),
            pltpu.VMEM((Y, 3, 128, 8), f32),
            pltpu.VMEM((2, 3, 1, 512), f32),
            pltpu.VMEM((3, 8, 128), f32),
            dma((4,)),
            dma, dma((n,)), dma((2,)), dma,
            dma, dma, dma, dma, dma((2,)), dma((2,)),
            dma, dma((1 + max(map(max, SIDE_AT)),)), dma, dma, dma((1 + max(map(max, CORE_AT)),)),
            dma, dma((1 + max(map(max, LONG_AT)),)), dma, dma((1 + max(map(max, SHORT_AT)),)),
            dma, dma((2,)), dma((ENDS, 2)),
        ],
        compiler_params=pltpu.CompilerParams(has_side_effects=True, collective_id=0, vmem_limit_bytes=44 * 2**20),
    )(pltpu.with_memory_space_constraint(dosages, pltpu.HBM))


def solution(mesh):
    return jax.shard_map(
        shards,
        mesh=mesh,
        in_specs=(P("samp", ("win", "snp")),),
        out_specs=(P("win", "samp", "snp"), P("win", "samp", "snp")),
        check_vma=False,
    )
```

```python
import jax
import jax.numpy as jnp
from jax import lax
from jax.experimental import pallas as pl
from jax.experimental.pallas import tpu as pltpu
from jax.sharding import PartitionSpec as P

MESH = pl.DeviceIdType.MESH


Z, Y = 8, 4
SAMPLES = 8192
HERE = 1024
HALF = 512
FLOOR = 0.05
POWER = 15
SCALE = 2.0 ** (126.5 / POWER)
FIRST = (0, 32, 64, 128, 192, 256, 320, 384, 448)
ROWS = (32, 32, 64, 64, 64, 64, 64, 64, 64)
PARTS = (
    (0, 32, 0, 256), (0, 32, 256, 256), (32, 32, 0, 256), (32, 32, 256, 256), (64, 64, 0, 256), (64, 64, 256, 256),
    (128, 32, 0, 512), (160, 32, 0, 512), (192, 32, 0, 512), (224, 32, 0, 512), (256, 32, 0, 512),
    (288, 32, 0, 512), (320, 32, 0, 512), (352, 32, 0, 512), (384, 32, 0, 512), (416, 32, 0, 512),
    (448, 32, 0, 512), (480, 32, 0, 512), (576, 32, 0, 512), (608, 32, 0, 512), (512, 32, 0, 512),
    (544, 32, 0, 512),
)
ENDS = max(sum((r // 256 if r < 512 else (r - 512) // 64) == h for r, _, _, _ in PARTS) for h in range(2))
TURN = sum(row < 128 for row in FIRST)
LONG_AT = (
    (0, 2, 3, 4, 5, 6, 12, 13, 2, 15, 8, 9, 1, 3, 15, 16, 7, 17, 8, 9, 10, 1),
    (1, 0, 8, 9, 10, 11, 6, 16, 10, 11, 4, 5, 14, 0, 11, 13, 5, 2, 6, 4, 15, 0),
    (7, 14, 1, 3, 4, 5, 0, 13, 6, 2, 12, 18, 19, 3, 14, 16, 18, 8, 9, 7, 12, 17),
)
SHORT_AT = (
    (0, 2, 3, 4, 5, 6, 11, 12, 5, 4, 10, 9, 0, 2, 5, 12, 9, 8, 10, 1, 13, 0),
    (1, 0, 7, 8, 9, 10, 6, 3, 8, 11, 7, 6, 3, 4, 11, 14, 7, 2, 6, 15, 16, 3),
)
SIDE_AT = (
    (0, 2, 4, 8, 11, 1, 12, 6, 10),
    (1, 3, 7, 10, 0, 3, 5, 9, 0),
    (5, 6, 9, 2, 4, 8, 11, 1, 12),
)
CORE_AT = (
    (0, 1, 2, 3, 4, 0, 2, 8, 6),
    (5, 6, 5, 0, 6, 7, 6, 7, 6),
    (1, 7, 7, 5, 0, 5, 0, 5, 0),
)

bf16, f32 = jnp.bfloat16, jnp.float32


def coded(w):
    w2 = w * w
    w3 = w2 * w
    w6 = w3 * w3
    w12 = w6 * w6
    return (w12 * w3).astype(bf16)


def decoded(u):
    u = u.astype(f32)
    size = jnp.exp2(jnp.log2(jnp.abs(u)) * (1.0 / POWER))
    return jnp.where(u < 0, -size, size)


def kernel(
    x_hbm, out_ref, band_ref,
    x, xt, cols, own, prev, prods, long_in, long_out, short_in, short_out, own_out, ends,
    st1, st2, st3, rowv, colv, lanes,
    load_sem, x_send, x_recv, p_send, p_recv,
    s1_send, s1_recv, s2_send, s2_recv, s3_send, s3_recv,
    d_send, d_recv, r_send, c_send, c_recv,
    l_send, l_recv, t_send, t_recv, o_send, b_send, e_recv,
):
    samp, win, y = lax.axis_index("samp"), lax.axis_index("win"), lax.axis_index("snp")
    z, hi = samp // 2, samp % 2
    lo, core = win // 2, win % 2

    def dev(z_, hi_, lo_, core_, y_):
        return (2 * z_ + hi_, 2 * lo_ + core_, y_)

    def remote(src, dst, send, recv, to):
        return pltpu.make_async_remote_copy(
            src_ref=src, dst_ref=dst, send_sem=send, recv_sem=recv, device_id=to, device_id_type=MESH
        )

    def go(copy):
        copy.start()

    def bytes_of(ref, sem):
        pltpu.make_async_copy(ref, ref, sem).wait()

    here = dev(z, hi, lo, core, y)
    partner = dev(z, core, 1 - lo, hi, y)
    sibling = dev(z, hi, lo, 1 - core, y)
    up, down = dev(z, hi, lo, core, (y + 1) % Y), dev(z, hi, lo, core, (y + 3) % Y)
    sign = 1 - 2 * core
    fwd, bwd = dev((z + 8 + sign) % Z, hi, lo, core, y), dev((z + 8 - sign) % Z, hi, lo, core, y)
    mine = pl.ds(pl.multiple_of(HALF * core, HALF), HALF)
    by_hi = pl.ds(pl.multiple_of(HALF * hi, HALF), HALF)

    def turn(a):
        xt[pl.ds(128 * a, 128)] = x[:, pl.ds(128 * a, 128)].T

    def load(first, count, k):
        part = pl.ds(128 * first, 128 * count)
        return pltpu.make_async_copy(x_hbm.at[:, part], x.at[:, part], load_sem.at[k])

    loads = [load(0, 1, 0), load(4, 1, 1), load(1, 3, 2), load(5, 3, 3)]
    for copy in loads:
        copy.start()
    barrier = pltpu.get_barrier_semaphore()
    greeted = [dev((z + k) % Z, hi, lo, core, y) for k in range(1, Z)]
    greeted += [dev(z, hi, lo, c, (y + k) % Y) for k in range(1, Y) for c in range(2)]
    greeted += [dev(z, hi ^ (k // 4), lo ^ (k // 2 % 2), core ^ (k % 2), y) for k in range(1, 8)]
    for near in greeted:
        pl.semaphore_signal(barrier, 1, device_id=near, device_id_type=MESH)
    for n in range(2):
        loads[n].wait()
        turn(4 * n)

    pl.semaphore_wait(barrier, len(greeted))

    def rows_of(q):
        return pl.ds(FIRST[q], ROWS[q])

    def x_copy(q, i):
        return remote(
            xt.at[pl.ds(HALF * i + FIRST[q], ROWS[q])], cols.at[2 * y + i, rows_of(q), by_hi],
            x_send, x_recv.at[q], partner,
        )

    def sx(q):
        if q == TURN:
            for a in (1, 5, 2, 6, 3, 7):
                turn(a)
        for i in range(2):
            go(x_copy(q, i))

    next_hi, next_lo = 1 - core, jnp.where(core == 0, 1 - lo, lo)

    def prev_copy(c):
        return remote(
            x.at[:, pl.ds(512 * c, 512)], prev.at[by_hi, :], p_send.at[c], p_recv,
            dev(z, next_hi, next_lo, c, y),
        )

    to_self = jnp.logical_and(hi == 0, core == 1)

    def prev_local():
        return pltpu.make_async_copy(x_hbm.at[:, pl.ds(512, 512)], prev.at[by_hi, :], p_recv)

    def pv():
        go(prev_copy(0))
        pl.when(jnp.logical_not(to_self))(lambda: prev_copy(1).start())
        pl.when(to_self)(lambda: prev_local().start())

    def s1_copy(k):
        return remote(
            st1.at[z], st1.at[z], s1_send, s1_recv, dev((z + k) % Z, hi, lo, core, y)
        )

    def d_copy(q, way, i):
        block = cols.at[2 * y + i, rows_of(q), mine]
        return remote(block, block, d_send, d_recv.at[SIDE_AT[way ^ i][q]], (up, down)[way])

    def r_copy(q, way):
        block = cols.at[2 * ((y + (3, 1)[way]) % Y) + way, rows_of(q), mine]
        return remote(block, block, r_send, d_recv.at[SIDE_AT[2][q]], (up, down)[way])

    def pair(q, k):
        return cols.at[pl.ds(2 * ((y + k) % Y), 2), rows_of(q), mine]

    def c_copy(q, k):
        return remote(pair(q, k), pair(q, k), c_send, c_recv.at[CORE_AT[(0, 1, 2, 1)[k]][q]], sibling)

    def ax(q):
        bytes_of(pair(q, 0), x_recv.at[q])
        go(c_copy(q, 0))

    def da(q):
        for way in range(2):
            go(d_copy(q, way, way))

    def db(q):
        for way in range(2):
            go(d_copy(q, way, 1 - way))

    def re(q):
        bytes_of(pair(q, 0), d_recv.at[SIDE_AT[0][q]])
        for way in range(2):
            go(r_copy(q, way))

    def ne(q):
        bytes_of(pair(q, 0), d_recv.at[SIDE_AT[1][q]])
        for k in (1, 3):
            go(c_copy(q, k))

    def fa(q):
        bytes_of(pair(q, 0), d_recv.at[SIDE_AT[2][q]])
        go(c_copy(q, 2))

    def s2_copy(yy, c):
        return remote(lanes, st2.at[y, hi], s2_send, s2_recv, dev(z, core, 1 - lo, c, yy))

    def s3_copy(c):
        return remote(
            lanes, st3.at[hi], s3_send.at[c], s3_recv.at[hi], dev(z, next_hi, next_lo, c, y)
        )

    def st_sums():
        for n in (2, 3):
            loads[n].wait()

        @pl.loop(0, 8)
        def _(a):
            v = x[:, pl.ds(pl.multiple_of(128 * a, 128), 128)].astype(f32)
            st1[z, 0, pl.ds(a, 1), :] = jnp.sum(v, axis=0, keepdims=True)
            st1[z, 1, pl.ds(a, 1), :] = jnp.sum(v * v, axis=0, keepdims=True)

        for k in range(1, Z):
            go(s1_copy(k))

    def st_send():
        bytes_of(st1.at[pl.ds(0, Z - 1)], s1_recv)
        total = st1[0]
        for k in range(1, Z):
            total = total + st1[k]
        lanes[0] = total[0]
        lanes[1] = total[1]
        lanes[2] = st1[z, 0]
        for c in range(2):
            for k in range(Y):
                go(s2_copy((y + k) % Y, c))
        go(s3_copy(0))
        pl.when(jnp.logical_not(to_self))(lambda: s3_copy(1).start())

        @pl.when(to_self)
        def _():
            st3[hi] = lanes[...]

    def of_sums(parts):
        total, square, local = (parts[k] for k in range(3))
        mean = total * (1.0 / SAMPLES)
        var = jnp.maximum(square * (1.0 / SAMPLES) - mean * mean, FLOOR)
        return mean, 1.0 / jnp.sqrt(var), local

    def st_finish():
        bytes_of(st2, s2_recv)

        for yy in range(Y):
            mean, inv, local = of_sums(st2[yy, 0] + st2[yy, 1])
            e = inv * (SCALE / SAMPLES)
            rowv[yy, 0] = e.T
            rowv[yy, 1] = (local * e).T
            rowv[yy, 2] = (mean * e).T

        def col_vectors(at, parts):
            mean, inv, local = of_sums(parts)
            lanes_of = (inv, mean * inv, (local - HERE * mean) * inv)
            for n, t in enumerate(lanes_of):
                half = jnp.where(core == 0, t[:4], t[4:])
                for j in range(4):
                    colv[at, n, :, pl.ds(128 * j, 128)] = half[j : j + 1]

        col_vectors(0, st2[y, 0] + st2[y, 1])
        for h in range(2):
            there = pltpu.make_async_copy(st3.at[h], st3.at[h], s3_recv.at[h])
            if h == 0:
                pl.when(jnp.logical_not(to_self))(there.wait)
            else:
                there.wait()
        col_vectors(1, st3[0] + st3[1])

    def st(k):
        (st_sums, st_send, st_finish)[k]()

    def ow(m):
        for q in range(len(FIRST)):
            if m == (FIRST[q] + ROWS[q] - 1) // 128:
                c_copy(q, 0).wait_recv()
        own[:, pl.ds(128 * m, 128)] = cols[2 * y + core, pl.ds(128 * m, 128)].T

    def products(left, right, size, yy, tiles, roots, at, inside, to, part):
        g = lax.dot_general(
            left.reshape(2 * size, HERE), right[:, part], (((1,), (0,)), ((), ())), preferred_element_type=f32
        )
        for i in range(2):
            e, s, m = (rowv[yy, n, pl.ds(inside, size), tiles[i] : tiles[i] + 1] for n in range(3))
            v = [colv[at, n, :, part] for n in range(3)]
            prods[roots[i], pl.ds(to, size), part] = g[size * i : size * i + size] * (e * v[0]) - s * v[1] - m * v[2]

    def main(q, ks, n):
        part = pl.ds(0, 512) if n is None else pl.ds(256 * n, 256)
        tile, inside = FIRST[q] // 128, FIRST[q] % 128
        for k in ks:
            yy = (y + k) % Y
            left = cols[pl.ds(2 * yy, 2), rows_of(q)]
            products(left, own, ROWS[q], yy, (tile, 4 + tile), (2 * yy, 2 * yy + 1), 0, inside, FIRST[q], part)

    def pn(q, n=None):
        if not n:
            bytes_of(cols.at[pl.ds(0, 4), rows_of(q), mine], c_recv.at[CORE_AT[1][q]])
        main(q, (0, 1, 3), n)

    def pa(q, n=None):
        main(q, (0, 1, 2, 3), n)

    def pf(q, n=None):
        if not n:
            c_copy(q, 2).wait_recv()
        main(q, (2,), n)

    def pb():
        bytes_of(prev, p_recv)
        for k in range(4):
            left = cols[0:2, pl.ds(128 * k, 128)]
            products(left, prev, 128, 0, (k, 4 + k), (k, 4 + k), 1, 0, 512, pl.ds(0, 512))

    def spot(u):
        row, tall, col, wide = PARTS[u]
        return pl.ds(row, tall), pl.ds(col, wide)

    def half_of(u):
        row = PARTS[u][0]
        return row // 256 if row < 512 else (row - 512) // 64

    def slot(u):
        return sum(half_of(n) == half_of(u) for n in range(u))

    def home(u, z_):
        if PARTS[u][0] < 512:
            return dev(z_, half_of(u), 1 - lo, hi, y)
        return dev(z_, half_of(u), jnp.where(hi == 1, 1 - lo, lo), 1 - hi, y)

    def at_home(u):
        row, tall, col, wide = PARTS[u]
        return pl.ds(row % 256 if row < 512 else 256 + (row - 512) % 64, tall), pl.ds(col, wide)

    def l_copy(t, u):
        r, c = spot(u)
        if t < 3:
            return remote(long_out.at[t, r, c], long_in.at[t, r, c], l_send, l_recv.at[LONG_AT[t][u]], fwd)
        hr, hc = at_home(u)
        return remote(
            long_out.at[t, r, c], ends.at[0, core, hr, hc], l_send, e_recv.at[slot(u)],
            home(u, (z + 8 + sign) % Z),
        )

    def t_copy(t, u):
        r, c = spot(u)
        if t < 2:
            return remote(short_out.at[t, r, c], short_in.at[t, r, c], t_send, t_recv.at[SHORT_AT[t][u]], bwd)
        hr, hc = at_home(u)
        return remote(
            short_out.at[t, r, c], ends.at[1, core, hr, hc], t_send, e_recv.at[slot(u)],
            home(u, (z + 8 - sign) % Z),
        )

    def L(t, u):
        r, c = spot(u)
        if t:
            l_copy(t - 1, u).wait_recv()
        w = prods[(z + 8 + sign * (4 - t)) % Z, r, c]
        if t:
            w = w + decoded(long_in[t - 1, r, c])
        long_out[t, r, c] = coded(w)
        go(l_copy(t, u))

    def S(t, u):
        r, c = spot(u)
        if t:
            t_copy(t - 1, u).wait_recv()
        w = prods[(z + 8 - sign * (3 - t)) % Z, r, c]
        if t:
            w = w + decoded(short_in[t - 1, r, c])
        short_out[t, r, c] = coded(w)
        go(t_copy(t, u))

    def local_end(u):
        return PARTS[u][0] >= 512 and half_of(u) == 0

    def O(u):
        r, c = spot(u)
        hr, hc = at_home(u)
        own_out[r, c] = coded(prods[z, r, c])
        main_part = PARTS[u][0] < 512
        copy = remote(
            own_out.at[r, c], ends.at[2, core, hr, hc], o_send if main_part else b_send.at[half_of(u)],
            e_recv.at[slot(u)], home(u, z),
        )
        if local_end(u):
            pl.when(jnp.logical_not(to_self))(copy.start)

            @pl.when(to_self)
            def _():
                ends[2, 1, hr, hc] = own_out[r, c]
        else:
            copy.start()

    def F(u):
        @pl.when(hi == half_of(u))
        def _():
            row, tall, col, wide = PARTS[u]
            hr, hc = at_home(u)
            if local_end(u):
                pl.when(to_self)(lambda: bytes_of(ends.at[0, 0, pl.ds(0, 5 * tall), pl.ds(0, wide)], e_recv.at[slot(u)]))

                @pl.when(jnp.logical_not(to_self))
                def _():
                    bytes_of(ends.at[:, :, pl.ds(0, tall), pl.ds(0, wide)], e_recv.at[slot(u)])
            else:
                bytes_of(ends.at[:, :, pl.ds(0, tall), pl.ds(0, wide)], e_recv.at[slot(u)])
            for c in range(2):
                w = sum(decoded(ends[n, c, hr, hc]) for n in range(3))
                value = w * w * (1.0 / (SCALE * SCALE))
                there = pl.ds(HALF * c + col, wide)
                if row < 512:
                    out_ref[0, pl.ds(row % 256, tall), there] = value
                else:
                    band_ref[0, pl.ds((row - 512) % 64, tall), there] = value

    plan = [
        (sx, 0), (sx, 1), (sx, 2), (st, 0), (sx, 3), (sx, 4), (ax, 0), (da, 0), (db, 0), (ax, 1), (da, 1), (db, 1),
        (st, 1), (sx, 5), (sx, 6), (sx, 7), (sx, 8), (ax, 2), (da, 2), (ax, 3), (ow, 0), (re, 0), (ax, 4), (ne, 0),
        (re, 1), (db, 2), (da, 3), (ne, 1), (ow, 1), (ax, 5), (st, 2), (re, 2), (db, 3), (da, 4), (fa, 0),
        (pn, 0, 0), (ax, 6), (pn, 1, 0), (fa, 1), (ax, 7), (pf, 0, 0), (L, 0, 0), (S, 0, 0), (O, 0), (ow, 2),
        (ne, 2), (pf, 1, 0), (ax, 8), (pv,), (re, 3), (db, 4), (da, 5), (pn, 2, 0), (ow, 3), (L, 1, 0), (fa, 2),
        (S, 1, 0), (pa, 0, 1), (L, 0, 1), (S, 0, 1), (L, 0, 2), (S, 0, 2), (pa, 1, 1), (L, 0, 3), (ne, 3), (S, 0, 3),
        (O, 1), (O, 2), (O, 3), (pf, 2, 0), (L, 0, 4), (S, 0, 4), (pa, 2, 1), (re, 4), (db, 5), (da, 6), (L, 0, 5),
        (S, 0, 5), (L, 2, 0), (S, 2, 0), (O, 4), (O, 5), (pn, 3), (fa, 3), (L, 1, 1), (S, 1, 1), (L, 1, 2),
        (S, 1, 2), (L, 1, 3), (S, 1, 3), (ne, 4), (L, 1, 4), (S, 1, 4), (pf, 3), (L, 1, 5), (S, 1, 5), (L, 0, 6),
        (S, 0, 6), (L, 0, 7), (L, 3, 0), (S, 0, 7), (O, 6), (O, 7), (re, 5), (db, 6), (da, 7), (L, 2, 1), (S, 2, 1),
        (L, 2, 2), (pn, 4), (fa, 4), (S, 2, 2), (L, 2, 3), (S, 2, 3), (L, 2, 4), (S, 2, 4), (ne, 5), (L, 2, 5),
        (S, 2, 5), (pf, 4), (L, 1, 6), (S, 1, 6), (L, 0, 8), (S, 0, 8), (L, 0, 9), (S, 0, 9), (O, 8), (O, 9),
        (re, 6), (db, 7), (da, 8), (L, 1, 7), (S, 1, 7), (pn, 5), (fa, 5), (L, 3, 1), (L, 3, 2), (L, 3, 3), (F, 0),
        (L, 3, 4), (ne, 6), (L, 3, 5), (pf, 5), (S, 2, 6), (L, 2, 6), (L, 0, 10), (S, 0, 10), (L, 0, 11), (S, 0, 11),
        (O, 10), (O, 11), (re, 7), (db, 8), (S, 1, 8), (L, 1, 8), (pn, 6), (fa, 6), (L, 1, 9), (S, 2, 7), (L, 2, 7),
        (S, 1, 9), (ne, 7), (F, 1), (F, 2), (F, 3), (pf, 6), (S, 1, 10), (L, 0, 12), (S, 0, 12), (L, 0, 13), (F, 4),
        (S, 0, 13), (re, 8), (L, 3, 6), (O, 12), (S, 1, 11), (O, 13), (F, 5), (L, 1, 10), (pn, 7), (fa, 7),
        (S, 2, 8), (L, 1, 11), (L, 2, 8), (S, 2, 9), (ne, 8), (L, 2, 9), (S, 2, 10), (pf, 7), (L, 3, 7), (S, 1, 12),
        (L, 0, 14), (S, 0, 14), (L, 0, 15), (S, 0, 15), (O, 14), (O, 15), (L, 1, 12), (S, 1, 13), (fa, 8), (pn, 8),
        (S, 2, 11), (L, 1, 13), (L, 2, 10), (pf, 8), (F, 6), (L, 0, 16), (S, 0, 16), (L, 0, 17), (L, 2, 11),
        (S, 0, 17), (pb,), (L, 3, 8), (L, 3, 9), (S, 2, 12), (S, 1, 14), (L, 0, 18), (S, 0, 18), (L, 0, 19),
        (S, 0, 19), (L, 0, 20), (S, 0, 20), (S, 1, 15), (O, 16), (O, 17), (O, 18), (O, 19), (O, 20), (L, 1, 14),
        (S, 2, 13), (F, 7), (L, 0, 21), (S, 0, 21), (O, 21), (L, 1, 15), (L, 2, 12), (S, 1, 16), (L, 2, 13),
        (S, 1, 17), (L, 3, 10), (L, 1, 16), (S, 2, 14), (L, 1, 17), (S, 1, 18), (L, 3, 11), (S, 1, 19), (S, 1, 20),
        (S, 2, 15), (F, 8), (L, 1, 18), (F, 9), (L, 1, 19), (S, 1, 21), (L, 1, 20), (S, 2, 16), (L, 2, 14),
        (S, 2, 17), (L, 1, 21), (L, 2, 15), (S, 2, 18), (L, 3, 12), (S, 2, 19), (L, 3, 13), (S, 2, 20), (L, 2, 16),
        (S, 2, 21), (F, 10), (L, 2, 17), (L, 2, 18), (F, 11), (L, 2, 19), (L, 2, 20), (L, 3, 14), (L, 2, 21),
        (L, 3, 15), (L, 3, 16), (L, 3, 17), (F, 12), (L, 3, 18), (F, 13), (L, 3, 19), (L, 3, 20), (L, 3, 21),
        (F, 14), (F, 15), (F, 16), (F, 17), (F, 18), (F, 19), (F, 20), (F, 21),
    ]
    for step, *at in plan:
        with jax.named_scope("_".join((step.__name__, *map(str, at)))):
            step(*at)

    def close():
        bytes_of(xt, x_send)
        bytes_of(cols.at[pl.ds(0, 4), :, mine], d_send)
        bytes_of(cols.at[pl.ds(0, 2), :, mine], r_send)
        bytes_of(cols.at[:, :, mine], c_send)
        bytes_of(st1.at[pl.ds(0, Z - 1)], s1_send)
        bytes_of(st2, s2_send)
        bytes_of(long_out, l_send)
        bytes_of(short_out, t_send)
        bytes_of(own_out.at[pl.ds(0, 512)], o_send)
        bytes_of(own_out.at[pl.ds(576, 64)], b_send.at[1])
        prev_copy(0).wait_send()
        s3_copy(0).wait_send()

        @pl.when(jnp.logical_not(to_self))
        def _():
            prev_copy(1).wait_send()
            s3_copy(1).wait_send()
            bytes_of(own_out.at[pl.ds(512, 64)], b_send.at[0])

    with jax.named_scope("close"):
        close()


def shards(dosages):
    vmem = pl.BlockSpec(memory_space=pltpu.VMEM)
    dma = pltpu.SemaphoreType.DMA
    n = len(FIRST)
    return pl.pallas_call(
        kernel,
        name="ld",
        out_shape=(
            jax.ShapeDtypeStruct((1, 256, 1024), f32),
            jax.ShapeDtypeStruct((1, 64, 1024), f32),
        ),
        in_specs=[pl.BlockSpec(memory_space=pltpu.HBM)],
        out_specs=(vmem, vmem),
        scratch_shapes=[
            pltpu.VMEM((HALF, 1024), bf16),
            pltpu.VMEM((1024, HALF), bf16),
            pltpu.VMEM((Z, 512, HERE), bf16),
            pltpu.VMEM((HERE, 512), bf16),
            pltpu.VMEM((HERE, 512), bf16),
            pltpu.VMEM((Z, 640, 512), f32),
            pltpu.VMEM((3, 640, 512), bf16),
            pltpu.VMEM((4, 640, 512), bf16),
            pltpu.VMEM((2, 640, 512), bf16),
            pltpu.VMEM((3, 640, 512), bf16),
            pltpu.VMEM((640, 512), bf16),
            pltpu.VMEM((3, 2, 320, 512), bf16),
            pltpu.VMEM((Z, 2, 8, 128), f32),
            pltpu.VMEM((Y, 2, 3, 8, 128), f32),
            pltpu.VMEM((2, 3, 8, 128), f32),
            pltpu.VMEM((Y, 3, 128, 8), f32),
            pltpu.VMEM((2, 3, 1, 512), f32),
            pltpu.VMEM((3, 8, 128), f32),
            dma((4,)),
            dma, dma((n,)), dma((2,)), dma,
            dma, dma, dma, dma, dma((2,)), dma((2,)),
            dma, dma((1 + max(map(max, SIDE_AT)),)), dma, dma, dma((1 + max(map(max, CORE_AT)),)),
            dma, dma((1 + max(map(max, LONG_AT)),)), dma, dma((1 + max(map(max, SHORT_AT)),)),
            dma, dma((2,)), dma((ENDS,)),
        ],
        compiler_params=pltpu.CompilerParams(has_side_effects=True, collective_id=0, vmem_limit_bytes=44 * 2**20),
    )(pltpu.with_memory_space_constraint(dosages, pltpu.HBM))


def solution(mesh):
    return jax.shard_map(
        shards,
        mesh=mesh,
        in_specs=(P("samp", ("win", "snp")),),
        out_specs=(P("win", "samp", "snp"), P("win", "samp", "snp")),
        check_vma=False,
    )
```
